512 devices in a mesh: row: 32 (over y, x), col: 16 (over z, core).
Axes of the slice: x: 4, y: 8, z: 8, core: 2. Of those that a mesh axis runs over, the one named last changes fastest.
Arguments:
- state: float32 [8192, 16, 1024], P('row', 'col'), may hold values from -6 to 6
- coupling: bfloat16 [8192, 16, 1024], P('row', 'col'), may hold values from -2 to 2, as said below
- coupling_t: bfloat16 [2, 8192, 16, 1024], P(None, 'row', 'col'), may hold values from -2 to 2, as said below
- factor: float32 [4, 16, 256, 256], P(None, 'col', 'row'), may hold values from -0.3 to 1.3
- cofactor: float32 [4, 16, 256, 256], P(None, 'col', 'row'), may hold values from -0.3 to 1.3
- rates: float32 [4, 16, 256], P(None, 'col'), may hold values from 0.5 to 2
Outputs:
- updated_state: float32 [8192, 16, 1024], P('row', 'col')
The draws below stay inside these ranges and needn't reach their ends.
Inputs may be any that keep to these rules, and one draw needn't show every extreme that they name: coupling and coupling_t hold the same matrix A; its blocks A(i, k) are zero unless k > i. coupling_t holds the transposed blocks of the A in coupling.
All inputs are finite; a program needn't handle non-finite values.
Results may differ from the reference program's by a relative error of at most 0.0003.
Values may be sent and summed in bfloat16 or wider, within the bound.
A program may use at most 64 MiB of HBM per device.

```python
import math
import jax
import jax.numpy as jnp
from jax import lax

BS = 256
STEPS = 2
NBH = 32
NB = 64
CB = 4
N_COL = 16


def coupling_blocks(seed_key, block_rows, block_cols):
    base_key = jax.random.fold_in(seed_key, 404)
    flat_rows = block_rows.reshape(-1).astype(jnp.int32)
    flat_cols = block_cols.reshape(-1).astype(jnp.int32)
    limit = 4.0 / math.sqrt(BS)

    def one_block(row_id, col_id):
        sub_key = jax.random.fold_in(base_key, row_id * NB + col_id)
        values = jax.random.normal(sub_key, (BS, BS), jnp.float32) / math.sqrt(BS)
        values = jnp.clip(values, -limit, limit)
        return jnp.where(col_id > row_id, values, 0.0)
    drawn = jax.vmap(one_block)(flat_rows, flat_cols)
    return drawn.reshape(block_rows.shape + (BS, BS))


def draw_coupling(key, part):
    col_count = NB // CB
    row_ids = jnp.arange(NBH, dtype=jnp.int32)[:, None, None]
    stored = (jnp.arange(CB, dtype=jnp.int32)[:, None] * col_count + jnp.arange(col_count, dtype=jnp.int32)[None, :])[None]
    block_rows = jnp.broadcast_to(row_ids, (NBH, CB, col_count))
    block_cols = jnp.broadcast_to(NB - 1 - stored, (NBH, CB, col_count))
    drawn = coupling_blocks(key, block_rows, block_cols)
    drawn = jnp.transpose(drawn, (0, 3, 2, 1, 4))
    return drawn.reshape(NBH * BS, col_count, CB * BS).astype(jnp.bfloat16)


def draw_coupling_t(key, part):
    col_count = NB // CB
    rotated = (jnp.arange(NBH, dtype=jnp.int32) + NBH // 2) % NBH
    stored_rows = jnp.arange(2, dtype=jnp.int32)[:, None] * NBH + rotated[None, :]
    stored_cols = jnp.arange(CB, dtype=jnp.int32)[:, None] * col_count + jnp.arange(col_count, dtype=jnp.int32)[None, :]
    block_rows = jnp.broadcast_to(stored_cols[None, None], (2, NBH, CB, col_count))
    block_cols = jnp.broadcast_to((NB - 1 - stored_rows)[:, :, None, None], (2, NBH, CB, col_count))
    drawn = coupling_blocks(key, block_rows, block_cols)
    drawn = jnp.swapaxes(drawn, -1, -2)
    drawn = jnp.transpose(drawn, (0, 1, 4, 3, 2, 5))
    return drawn.reshape(2, NBH * BS, col_count, CB * BS).astype(jnp.bfloat16)


def operator_draw(seed_key):
    col_count = NB // CB
    perturb = jax.random.normal(seed_key, (CB, col_count, BS, BS), jnp.float32)
    perturb = jnp.clip(0.3 * perturb / math.sqrt(BS), -0.3, 0.3)
    return jnp.eye(BS, dtype=jnp.float32) + perturb


def draw_factor(key, part):
    return operator_draw(jax.random.fold_in(key, 17))


def draw_cofactor(key, part):
    return operator_draw(jax.random.fold_in(key, 29))


def block_scale(own_key, dims, shards, least, largest):
    gain = 1.0
    for axis_at, blocks in shards:
        steps = jax.random.uniform(jax.random.fold_in(jax.random.fold_in(own_key, 6), axis_at), (blocks,), jnp.float32, least / len(shards), largest / len(shards))
        gain = gain * jnp.repeat(jnp.exp(steps), dims[axis_at] // blocks).reshape((-1,) + (1,) * (len(dims) - 1 - axis_at))
    return gain


def centred(stream_key, dims, scale, bound, pieces=(), held_as=jnp.bfloat16):
    entries = jax.random.normal(stream_key, dims, jnp.float32) * scale
    if len(pieces) > 0:
        entries = block_scale(stream_key, dims, pieces, -0.22, 0.18) * entries
    return jnp.clip(entries, min=-bound, max=bound).astype(held_as)


def setup_inputs(seed: int = 0) -> dict:
    key_list = jax.random.split(jax.random.key(seed), 7)
    state = centred(key_list[0], (NBH * BS, N_COL, CB * BS), 1.0, 6.0, ((0, 32), (1, 16)), jnp.float32)
    coupling = draw_coupling(jax.random.fold_in(key_list[6], 71), 0)
    coupling_t = draw_coupling_t(jax.random.fold_in(key_list[6], 71), 0)
    factor = draw_factor(jax.random.fold_in(key_list[6], 71), 0)
    cofactor = draw_cofactor(jax.random.fold_in(key_list[6], 71), 0)
    rates = jnp.clip(jnp.exp(math.log(2.0) - 1.3862944 * jax.random.uniform(key_list[5], (CB, N_COL, BS), jnp.float32) ** block_scale(key_list[5], (CB, N_COL, BS), ((1, 16),), -0.2, 0.2)), 0.5, 2.0)
    return {"state": state, "coupling": coupling, "coupling_t": coupling_t, "factor": factor, "cofactor": cofactor, "rates": rates}


HIGHEST_PRECISION = lax.Precision.HIGHEST


def to_blocks(flattened, row_total):
    col_count = flattened.shape[1]
    shaped = flattened.reshape(row_total, BS, col_count, CB, BS)
    shaped = jnp.transpose(shaped, (0, 3, 2, 1, 4))
    return shaped.reshape(row_total, CB * col_count, BS, BS)


def from_blocks(blocks):
    row_total = blocks.shape[0]
    col_count = blocks.shape[1] // CB
    shaped = blocks.reshape(row_total, CB, col_count, BS, BS)
    shaped = jnp.transpose(shaped, (0, 3, 2, 1, 4))
    return shaped.reshape(row_total * BS, col_count, CB * BS)


def solve_block(residual, left_p, left_q, left_e, right_p, right_q, right_e):
    middle = jnp.dot(left_q, residual, precision=HIGHEST_PRECISION, preferred_element_type=jnp.float32)
    middle = jnp.dot(middle, right_q.T, precision=HIGHEST_PRECISION, preferred_element_type=jnp.float32)
    middle = middle / (left_e[:, None] + right_e[None, :])
    product = jnp.dot(left_p, middle, precision=HIGHEST_PRECISION, preferred_element_type=jnp.float32)
    return -jnp.dot(product, right_p.T, precision=HIGHEST_PRECISION, preferred_element_type=jnp.float32)


def reference(state, coupling, coupling_t, factor, cofactor, rates):
    col_count = state.shape[1]
    half_rows = NBH // 2
    blocks = to_blocks(state, NBH)
    upper_blocks = to_blocks(coupling, NBH)
    lower_blocks = to_blocks(coupling_t.reshape(NB * BS, col_count, CB * BS), NB)
    all_p = factor.reshape(NB, BS, BS)
    all_q = cofactor.reshape(NB, BS, BS)
    all_e = rates.reshape(NB, BS)
    row_ids = jnp.arange(NBH, dtype=jnp.int32)
    col_ids = jnp.arange(NB, dtype=jnp.int32)
    for wave_step in range(STEPS):
        antidiag = NB - 1 - wave_step
        partner = (antidiag - row_ids).astype(jnp.int32)
        usable = row_ids <= partner
        residual = blocks[row_ids, partner]
        solution = jax.vmap(solve_block)(residual, all_p[:NBH], all_q[:NBH], all_e[:NBH], all_p[partner], all_q[partner], all_e[partner])
        solution = jnp.where(usable[:, None, None], solution, 0.0)
        blocks = blocks.at[row_ids, partner].set(jnp.where(usable[:, None, None], solution, residual))
        mirror = (antidiag - col_ids).astype(jnp.int32)
        use_row = mirror <= col_ids
        sources = jnp.clip(jnp.where(use_row, mirror, col_ids), 0, NBH - 1).astype(jnp.int32)
        chosen = solution[sources]
        partner_blocks = jnp.where(use_row[:, None, None], chosen, jnp.swapaxes(chosen, 1, 2))
        upper_pick = jnp.clip(wave_step + col_ids, 0, NB - 1).astype(jnp.int32)

        def update_row(row_args, wave_step=wave_step, antidiag=antidiag, partner_blocks=partner_blocks, upper_pick=upper_pick):
            row_id, row_blocks, row_solution = row_args
            needed = wave_step + row_id
            stored = ((needed % NBH + half_rows) % NBH + NBH * (needed // NBH)).astype(jnp.int32)
            coupled = upper_blocks[row_id][upper_pick].astype(jnp.float32)
            transposed = lower_blocks[stored].astype(jnp.float32)
            left_terms = jnp.einsum("mab,mbc->mac", coupled, partner_blocks, precision=HIGHEST_PRECISION)
            right_terms = jnp.einsum("ab,mbc->mac", row_solution, transposed, precision=HIGHEST_PRECISION)
            targets = (row_id <= col_ids) & (row_id + col_ids < antidiag)
            return row_blocks - jnp.where(targets[:, None, None], left_terms + right_terms, 0.0)

        blocks = lax.map(update_row, (row_ids, blocks, solution))
    return from_blocks(blocks)
```

```python
import functools

import jax
import jax.numpy as jnp
from jax import lax
from jax.experimental import pallas as pl
from jax.experimental.pallas import tpu as pltpu
from jax.sharding import PartitionSpec as P

MESH = pl.DeviceIdType.MESH
STEPS = 2
XS = 4
BS = 256


def split2(a):
    hi = a.astype(jnp.bfloat16)
    return hi, (a - hi.astype(jnp.float32)).astype(jnp.bfloat16)


def nn(a, b):
    return lax.dot_general(a, b, (((1,), (0,)), ((), ())), preferred_element_type=jnp.float32)


def nt(a, b):
    return lax.dot_general(a, b, (((1,), (1,)), ((), ())), preferred_element_type=jnp.float32)


def dot3(dot, a, b):
    ah, al = split2(a)
    bh, bl = split2(b)
    return dot(ah, bh) + dot(ah, bl) + dot(al, bh)


def kernel(
    rows, cols, slots,
    st_in, cp_in, ct_in, p_in, q_in, e_in, out,
    st, w, a0, a1, at0, at1, pq, es, el, xr, zs,
    loc_sem, pq_ssem, pq_rsem, e_ssem, e_rsem,
    at_ssem, at0_rsem, atf_ssem, at1_rsem, a1_ssem, a1_rsem,
    xr_ssem, xr_rsem, z_ssem, z_rsem, root_ssem,
):
    r, c = lax.axis_index("row"), lax.axis_index("col")
    y, x = r // XS, lax.rem(r, XS)
    nb = 2 * rows
    pending = []

    def send(pred, src, dst, ssem, rsem, dev):
        cp = pltpu.make_async_remote_copy(
            src_ref=src, dst_ref=dst, send_sem=ssem, recv_sem=rsem,
            device_id=dev, device_id_type=MESH,
        )
        pl.when(pred)(cp.start)
        pending.append((pred, cp))

    def arrived(pred, dst, rsem):
        cp = pltpu.make_async_copy(dst, dst, rsem)
        pl.when(pred)(cp.wait)

    true = r >= 0
    sc = [lax.rem(nb - 1 - s - r, cols) for s in range(STEPS)]
    us = [(nb - 1 - s - r) // cols for s in range(STEPS)]
    is_s = [c == sc[s] for s in range(STEPS)]
    tcol, tslot = lax.rem(r, cols), r // cols

    ld_st = pltpu.make_async_copy(st_in, st, loc_sem.at[0])
    ld_st.start()
    ld_a0 = [
        pltpu.make_async_copy(cp_in.at[:, pl.ds(u * BS, BS)], a0.at[u], loc_sem.at[1 + u])
        for u in range(slots)
    ]
    for cp in ld_a0:
        cp.start()

    es[...] = jnp.broadcast_to(e_in[...], es.shape)

    def to_solver(s, side, q):
        if side == 0:
            m = c + cols * q
            slot = q
            dr, dc = m, lax.rem(nb - 1 - s - m, cols)
        else:
            m = c + cols * (2 + q)
            if s == 1:
                m = m - jnp.where(c == cols - 1, cols, 0)
            slot = m // cols
            dr, dc = nb - 1 - s - m, c
        mine = (dr == r) & (dc == c)
        for t, ref in enumerate((p_in, q_in)):
            src = ref.at[slot]
            dst = pq.at[s, side, t, pl.ds(pl.multiple_of(r * 8, 8), 8), :]
            send(~mine, src, dst, pq_ssem.at[s, side, q, t], pq_rsem.at[s, side], (dr, dc))
            pl.when(mine)(pltpu.make_async_copy(src, dst, pq_rsem.at[s, side]).start)

    def rate_to_solver(s):
        have = c == tcol
        mine = c == sc[s]
        send(have & ~mine, es.at[tslot], el.at[s], e_ssem.at[s], e_rsem.at[s], (r, sc[s]))
        pl.when(have & mine)(pltpu.make_async_copy(es.at[tslot], el.at[s], e_rsem.at[s]).start)

    for s in range(STEPS):
        for side in range(2):
            for q in range(2):
                to_solver(s, side, q)
        rate_to_solver(s)

    def at_needed(g, u):
        m = c + cols * u
        return (m >= g - 1) & (m <= nb - 2 - g)

    g = lax.rem(r + rows // 2, rows)
    for u in reversed(range(slots)):
        send(at_needed(g, u), ct_in.at[0, :, pl.ds(u * BS, BS)], at0.at[u],
             at_ssem.at[u], at0_rsem.at[u], (g, c))

    c_dn = lax.rem(c + cols - 1, cols)

    def step1_target(row, m):
        return (row <= m) & (row + m < nb - 2)

    for u in range(slots):
        wrap = jnp.where(c == 0, 1, 0)
        du = u - wrap
        send((du >= 0) & step1_target(r, c_dn + cols * du), cp_in.at[:, pl.ds(u * BS, BS)],
             a1.at[jnp.maximum(du, 0)], a1_ssem.at[u], a1_rsem.at[jnp.maximum(du, 0)], (r, c_dn))

    ld_st.wait()
    for u in range(slots):
        w[u] = st[:, 0, u * BS:(u + 1) * BS]
    for cp in ld_a0:
        cp.wait()

    def col_of(s, u):
        d = nb - 1 - s
        m = c + cols * u
        j = jnp.minimum(m, d - m)
        return d, m, j, m <= d

    def solver_sends(s):
        on = is_s[s]
        for h in range(2):
            if s == 0:
                send(on, xr.at[s, h], xr.at[s, h], xr_ssem.at[s, h, 3], xr_rsem.at[s, h], (r, sc[1]))
        for h in range(2):
            send(on & (c != tcol), xr.at[s, h], zs.at[s, tslot, h], root_ssem.at[s, h],
                 z_rsem.at[s, tslot, h], (r, tcol))

    def col_forward(s, u, on, wait=True):
        d, m, j, valid = col_of(s, u)
        yj, xj = j // XS, lax.rem(j, XS)
        root = valid & (r == j) & on
        own = is_s[s] & (u == us[s])
        if s == 1:
            own = own | (is_s[s] & (r == c + cols * u) & (c == tcol))
        holds = valid & (y <= yj) & on
        for h in range(2):
            buf, rs = zs.at[s, u, h], z_rsem.at[s, u, h]
            if wait:
                arrived(holds & ~own, buf, rs)

            def go(kind, pred, dev):
                send(pred, buf, buf, z_ssem.at[s, u, h, kind], rs, dev)

            direct = (u >= 2) if s == 0 else jnp.bool_(False)
            go(5, root & direct & (xj == 0) & (j >= 1), (jnp.maximum(j - 1, 0), c))
            for kind, dx in ((2, 3), (0, 1), (1, 2)):
                go(kind, root, (yj * XS + lax.rem(xj + dx, XS), c))
            dist = yj - y
            down = (dist >= 0) & (y >= 1) & (dist + 1 <= 4)
            skip = (dist == 0) & direct & (xj == 0) & (x == XS - 1)
            go(3, holds & down & ~skip, (jnp.maximum(r - XS, 0), c))
            first_up = (dist == 0) & (yj >= 5)
            next_up = (dist > 4) & (dist - 1 > 4)
            go(4, holds & (first_up | next_up), (jnp.where(first_up, x, lax.rem(r + XS, rows)), c))

    def row_forward(s):
        cs = sc[s]
        hz = lax.rem(c // 2 - cs // 2 + cols // 2, cols // 2)
        member = lax.rem(c, 2) == lax.rem(cs, 2)
        solver = is_s[s]
        mate = c + 1 - 2 * lax.rem(c, 2)
        early = is_s[1] if s == 0 else jnp.bool_(False)
        to_early = (mate == sc[1]) if s == 0 else jnp.bool_(False)
        half = cols // 4
        for h in range(2):
            arrived(~solver & ~early, xr.at[s, h], xr_rsem.at[s, h])

            def go(kind, pred, dc):
                send(pred, xr.at[s, h], xr.at[s, h], xr_ssem.at[s, h, kind], xr_rsem.at[s, h], (r, dc))

            go(0, member & (hz < half), lax.rem(c + 2, cols))
            go(1, member & ((hz == 0) | (hz > half + 1)), lax.rem(c + cols - 2, cols))
            go(2, member & ~to_early, mate)

    def solve(s):
        for side in range(2):
            pltpu.make_async_copy(pq.at[s, side], pq.at[s, side], pq_rsem.at[s, side]).wait()
        pltpu.make_async_copy(el.at[s], el.at[s], e_rsem.at[s]).wait()
        left_e = jnp.transpose(el[s])[:, :1]
        right_e = e_in[us[s]]
        mid = dot3(nn, pq[s, 0, 1], w[us[s]])
        mid = dot3(nt, mid, pq[s, 1, 1])
        mid = mid / (left_e + right_e)
        mid = dot3(nn, pq[s, 0, 0], mid)
        sol = -dot3(nt, mid, pq[s, 1, 0])
        hi, lo = split2(sol)
        xr[s, 0] = hi
        xr[s, 1] = lo
        if s == 0:
            zs[s, us[s], 0] = hi
            zs[s, us[s], 1] = lo
        else:
            last = r == rows - 1

            @pl.when(last)
            def _():
                th, tl = split2(jnp.transpose(sol))
                zs[s, us[s], 0] = th
                zs[s, us[s], 1] = tl

            @pl.when(~last)
            def _():
                zs[s, us[s], 0] = hi
                zs[s, us[s], 1] = lo

            @pl.when(~last & (c == tcol))
            def _():
                zs[s, tslot, 0] = hi
                zs[s, tslot, 1] = lo
        w[us[s]] = sol

    def terms(s, a, u, at, dot):
        z = zs.at[s, u]
        return dot(a, z[0]) + dot(a, z[1]) + nn(xr[s, 0], at) + nn(xr[s, 1], at)

    pl.when(is_s[0])(functools.partial(solve, 0))
    solver_sends(0)
    col_forward(0, us[0], is_s[0], wait=False)

    u1 = us[1]
    for h in range(2):
        arrived(is_s[1], xr.at[0, h], xr_rsem.at[0, h])
    col_forward(0, u1, is_s[1])
    arrived(is_s[1], at0.at[u1], at0_rsem.at[u1])

    @pl.when(is_s[1] & (r == rows - 1))
    def _():
        w[u1] = w[u1] - terms(0, a0[u1], u1, at0[u1], nt)

    @pl.when(is_s[1] & (r < rows - 1))
    def _():
        w[u1] = w[u1] - terms(0, a0[u1], u1, at0[u1], nn)

    pl.when(is_s[1])(functools.partial(solve, 1))
    solver_sends(1)
    col_forward(1, u1, is_s[1], wait=False)

    for u in reversed(range(slots)):
        arrived(at_needed(r, u) & ~(is_s[1] & (u == u1)), at0.at[u], at0_rsem.at[u])
        send(at_needed(r, u) & (r >= 1), at0.at[u], at1.at[u], atf_ssem.at[u], at1_rsem.at[u],
             (jnp.maximum(r - 1, 0), c))

    def update(s, a_ref, at_ref):
        for u in range(slots):
            m = c + cols * u
            target = (r <= m) & (r + m < nb - 1 - s)
            if s == 0:
                target = target & ~(is_s[1] & (u == u1))

            @pl.when(target)
            def _(u=u):
                w[u] = w[u] - terms(s, a_ref[u], u, at_ref[u], nt if u < 2 else nn)

    row_forward(0)
    for u in (2, 3, 1, 0):
        handled = (is_s[0] & (u == us[0])) | (is_s[1] & (u == u1))
        col_forward(0, u, ~handled)
    update(0, a0, at0)

    for u in (2, 3):
        col_forward(1, u, ~(is_s[1] & (u == u1)))
    row_forward(1)
    for u in (1, 0):
        col_forward(1, u, ~(is_s[1] & (u == u1)))
    for u in range(slots):
        need = step1_target(r, c + cols * u)
        arrived(need, a1.at[u], a1_rsem.at[u])
        arrived(at_needed(r + 1, u) & (r < rows - 1), at1.at[u], at1_rsem.at[u])
    update(1, a1, at1)
    for u in range(slots):
        out[:, 0, u * BS:(u + 1) * BS] = w[u]

    for pred, cp in pending:
        pl.when(pred)(cp.wait_send)


def solution(mesh):
    rows, cols = mesh.shape["row"], mesh.shape["col"]

    def on_device(state, coupling, coupling_t, factor, cofactor, rates):
        slots = 2 * rows // cols
        width = slots * BS
        any_space = pl.BlockSpec(memory_space=pl.ANY)
        vmem = pl.BlockSpec(memory_space=pltpu.VMEM)
        f32, bf16 = jnp.float32, jnp.bfloat16
        dma = pltpu.SemaphoreType.DMA
        return pl.pallas_call(
            functools.partial(kernel, rows, cols, slots),
            out_shape=jax.ShapeDtypeStruct((BS, 1, width), f32),
            in_specs=[any_space] * 5 + [vmem],
            out_specs=vmem,
            scratch_shapes=[
                pltpu.VMEM((BS, 1, width), f32),
                pltpu.VMEM((slots, BS, BS), f32),
                pltpu.VMEM((slots, BS, BS), bf16),
                pltpu.VMEM((slots, BS, BS), bf16),
                pltpu.VMEM((slots, BS, BS), bf16),
                pltpu.VMEM((slots, BS, BS), bf16),
                pltpu.VMEM((STEPS, 2, 2, BS, BS), f32),
                pltpu.VMEM((slots, 8, BS), f32),
                pltpu.VMEM((STEPS, 8, BS), f32),
                pltpu.VMEM((STEPS, 2, BS, BS), bf16),
                pltpu.VMEM((STEPS, slots, 2, BS, BS), bf16),
                dma((1 + slots,)),
                dma((STEPS, 2, 2, 2)),
                dma((STEPS, 2)),
                dma((STEPS,)),
                dma((STEPS,)),
                dma((slots,)),
                dma((slots,)),
                dma((slots,)),
                dma((slots,)),
                dma((slots,)),
                dma((slots,)),
                dma((STEPS, 2, 4)),
                dma((STEPS, 2)),
                dma((STEPS, slots, 2, 6)),
                dma((STEPS, slots, 2)),
                dma((STEPS, 2)),
            ],
            compiler_params=pltpu.CompilerParams(
                has_side_effects=True, vmem_limit_bytes=40 * 1024 * 1024
            ),
        )(
            state,
            coupling.reshape(BS, width),
            coupling_t.reshape(2, BS, width),
            factor.reshape(slots, 8, BS),
            cofactor.reshape(slots, 8, BS),
            rates,
        )

    return jax.shard_map(
        on_device,
        mesh=mesh,
        in_specs=(
            P("row", "col", None),
            P("row", "col", None),
            P(None, "row", "col", None),
            P(None, "col", "row", None),
            P(None, "col", "row", None),
            P(None, "col", None),
        ),
        out_specs=P("row", "col", None),
        check_vma=False,
    )
```

```python
import functools

import jax
import jax.numpy as jnp
from jax import lax
from jax.experimental import pallas as pl
from jax.experimental.pallas import tpu as pltpu
from jax.sharding import PartitionSpec as P

MESH = pl.DeviceIdType.MESH
STEPS = 2
XS = 4
BS = 256


def split2(a):
    hi = a.astype(jnp.bfloat16)
    return hi, (a - hi.astype(jnp.float32)).astype(jnp.bfloat16)


def nn(a, b):
    return lax.dot_general(a, b, (((1,), (0,)), ((), ())), preferred_element_type=jnp.float32)


def nt(a, b):
    return lax.dot_general(a, b, (((1,), (1,)), ((), ())), preferred_element_type=jnp.float32)


def dot3(dot, a, b):
    ah, al = split2(a)
    bh, bl = split2(b)
    return dot(ah, bh) + dot(ah, bl) + dot(al, bh)


def kernel(
    rows, cols, slots,
    st_in, cp_in, ct_in, p_in, q_in, e_in, out,
    st, w, a0, a1, at0, at1, pq, ev, es, el, xr, zs,
    loc_sem, pq_ssem, pq_rsem, e_ssem, e_rsem,
    at_ssem, at0_rsem, atf_ssem, at1_rsem, a1_ssem, a1_rsem,
    xr_ssem, xr_rsem, z_ssem, z_rsem, sv_ssem, er_ssem,
):
    r, c = lax.axis_index("row"), lax.axis_index("col")
    y, x = r // XS, lax.rem(r, XS)
    nb = 2 * rows
    pending = []

    def send(pred, src, dst, ssem, rsem, dev):
        cp = pltpu.make_async_remote_copy(
            src_ref=src, dst_ref=dst, send_sem=ssem, recv_sem=rsem,
            device_id=dev, device_id_type=MESH,
        )
        pl.when(pred)(cp.start)
        pending.append((pred, cp))

    def arrived(pred, dst, rsem):
        cp = pltpu.make_async_copy(dst, dst, rsem)
        pl.when(pred)(cp.wait)

    sc = [lax.rem(nb - 1 - s - r, cols) for s in range(STEPS)]
    us = [(nb - 1 - s - r) // cols for s in range(STEPS)]
    is_s = [c == sc[s] for s in range(STEPS)]
    tcol, tslot = lax.rem(r, cols), r // cols

    barrier = pltpu.get_barrier_semaphore()

    def greet(dr, dc):
        pl.semaphore_signal(barrier, inc=1, device_id=(dr, dc), device_id_type=MESH)

    ys = rows // XS
    for dx in range(1, XS):
        greet(y * XS + lax.rem(x + dx, XS), c)
    for dy in range(1, ys):
        greet(lax.rem(r + dy * XS, rows), c)
    greet(lax.rem(r + 1, rows), c)
    for dz in range(1, cols // 2):
        greet(r, lax.rem(c + 2 * dz, cols))
    greet(r, lax.rem(c + 1, cols))
    greet(r, c + 1 - 2 * lax.rem(c, 2))
    expected = XS - 1 + ys - 1 + 1 + cols // 2 - 1 + 2
    tj = y * XS + lax.rem(c, XS)
    near = lax.rem(y, cols // XS) == c // XS
    for s in range(STEPS):
        tj_col = lax.rem(nb - 1 - s - tj, cols)
        alone = (tj == r) & (tj_col == c)

        @pl.when(near & ~alone)
        def _(tj_col=tj_col):
            greet(tj, tj_col)

        expected = expected + jnp.where(is_s[s], XS, 0) - jnp.where(is_s[s] & (c == tcol), 1, 0)

        @pl.when(is_s[s])
        def _():
            for k in range(1, rows):
                greet(lax.rem(r + k, rows), c)

            for k in range(1, rows):
                greet(lax.rem(r + k, rows), tcol)

            @pl.when(c != tcol)
            def _():
                greet(r, tcol)

        expected = expected + 4 - jnp.where(is_s[s], 1, 0) - jnp.where(is_s[s] & (c == tcol), 1, 0)

    ld_st = pltpu.make_async_copy(st_in, st, loc_sem.at[0])
    ld_st.start()
    ld_a0 = [
        pltpu.make_async_copy(cp_in.at[:, pl.ds(u * BS, BS)], a0.at[u], loc_sem.at[1 + u])
        for u in range(slots)
    ]
    for cp in ld_a0:
        cp.start()
    ld_e = pltpu.make_async_copy(e_in, ev, loc_sem.at[1 + slots])
    ld_e.start()
    ld_e.wait()
    es[...] = jnp.broadcast_to(ev[...], es.shape)
    with jax.named_scope("barrier"):
        pl.semaphore_wait(barrier, expected)

    def to_solver(s, side, q):
        if side == 0:
            m = c + cols * q
            slot = q
            dr, dc = m, lax.rem(nb - 1 - s - m, cols)
        else:
            m = c + cols * (2 + q)
            if s == 1:
                m = m - jnp.where(c == cols - 1, cols, 0)
            slot = m // cols
            dr, dc = nb - 1 - s - m, c
        mine = (dr == r) & (dc == c)
        for t, ref in enumerate((p_in, q_in)):
            src = ref.at[slot]
            dst = pq.at[s, side, t, pl.ds(pl.multiple_of(r * 8, 8), 8), :]
            send(~mine, src, dst, pq_ssem.at[s, side, q, t], pq_rsem.at[s, side], (dr, dc))
            pl.when(mine)(pltpu.make_async_copy(src, dst, pq_rsem.at[s, side]).start)

    def rate_to_solver(s):
        have = c == tcol
        mine = c == sc[s]
        send(have & ~mine, es.at[tslot], el.at[s], e_ssem.at[s], e_rsem.at[s], (r, sc[s]))
        pl.when(have & mine)(pltpu.make_async_copy(es.at[tslot], el.at[s], e_rsem.at[s]).start)

    for s in range(STEPS):
        for side in range(2):
            for q in range(2):
                to_solver(s, side, q)
        rate_to_solver(s)

    for pred, cp in pending:
        pl.when(pred)(cp.wait_send)
    pending.clear()

    def at_needed(g, u):
        m = c + cols * u
        return (m >= g - 1) & (m <= nb - 2 - g)

    g = lax.rem(r + rows // 2, rows)
    for u in reversed(range(slots)):
        send(at_needed(g, u), ct_in.at[0, :, pl.ds(u * BS, BS)], at0.at[u],
             at_ssem.at[u], at0_rsem.at[u], (g, c))

    c_dn = lax.rem(c + cols - 1, cols)

    def step1_target(row, m):
        return (row <= m) & (row + m < nb - 2)

    for u in range(slots):
        wrap = jnp.where(c == 0, 1, 0)
        du = u - wrap
        send((du >= 0) & step1_target(r, c_dn + cols * du), cp_in.at[:, pl.ds(u * BS, BS)],
             a1.at[jnp.maximum(du, 0)], a1_ssem.at[u], a1_rsem.at[jnp.maximum(du, 0)], (r, c_dn))

    with jax.named_scope("local_in"):
        ld_st.wait()
        for u in range(slots):
            w[u] = st[:, 0, u * BS:(u + 1) * BS]
        for cp in ld_a0:
            cp.wait()

    def col_of(s, u):
        d = nb - 1 - s
        m = c + cols * u
        j = jnp.minimum(m, d - m)
        return d, m, j, m <= d

    def quarter(ref, q):
        return ref.at[:, pl.ds(pl.multiple_of(q * (BS // XS), BS // XS), BS // XS), :]

    def place(s, u):
        d = nb - 1 - s
        m = c + cols * u
        j = jnp.minimum(m, d - m)
        yj, xj = j // XS, lax.rem(j, XS)
        own_root = jnp.bool_(u >= 2) if isinstance(u, int) else u >= 2
        if s == 1:
            own_root = own_root | (lax.rem(j, cols // 2) == cols // 2 - 1)
        early = (j - 1) if s == 0 else j - 2 * rows
        early = jnp.where(u >= 2, early, -2 * rows)
        return j, yj, xj, m <= d, own_root, early

    def needed(s, u, row):
        j, yj, xj, valid, own_root, _ = place(s, u)
        return valid & ((row < j) | ((row == j) & ~own_root))

    def solver_sends(s):
        on = is_s[s]
        own = zs.at[s, us[s]]
        early = r - 1 if s == 0 else r - 2 * rows
        for k, dx in enumerate((3, 1, 2)):
            q = lax.rem(x + dx, XS)
            row = y * XS + q
            send(on & (row != early), quarter(own, q), quarter(own, q), sv_ssem.at[s, k],
                 z_rsem.at[s, us[s], q], (row, c))
        for q in range(XS):
            row = y * XS + q
            mine = (c == tcol) & (x == q)
            if s == 1:
                mine = mine | (r == rows - 1)
            send(on & ~mine, quarter(xr.at[s], q), quarter(zs.at[s, tslot], q), sv_ssem.at[s, 3 + q],
                 z_rsem.at[s, tslot, q], (row, tcol))

    def early_sends():
        on = is_s[0]
        send(on, xr.at[0], xr.at[0], er_ssem.at[XS], xr_rsem.at[0], (r, sc[1]))
        own = zs.at[0, us[0]]
        for q in range(XS):
            send(on & (r >= 1), quarter(own, q), quarter(own, q), er_ssem.at[q],
                 z_rsem.at[0, us[0], q], (jnp.maximum(r - 1, 0), c))

    def relay(s, u, on):
        j, yj, xj, valid, own_root, early = place(s, u)
        part = quarter(zs.at[s, u], x)
        first = on & valid & (y == yj)
        for y2 in range(ys - 1):
            row = y2 * XS + x
            send(first & (y2 < yj) & (row != early), part, part, z_ssem.at[s, u, y2],
                 z_rsem.at[s, u, x], (row, c))
        for k, dx in enumerate((1, 3, 2)):
            row = y * XS + lax.rem(x + dx, XS)
            send(on & needed(s, u, row) & (row != early), part, part, z_ssem.at[s, u, ys - 1 + k],
                 z_rsem.at[s, u, x], (row, c))

    def own_part(s, u):
        own = is_s[s] & (u == us[s])
        if s == 1:
            own = own | (is_s[s] & (c == tcol) & (u == tslot))
        return own

    def done_early(s, u):
        done = own_part(s, u)
        if s == 0:
            done = done | (is_s[1] & (u == u1) & (r < rows - 1))
        return done

    def relays(s, first):
        for u in (3, 0, 2, 1):
            j, yj, xj, valid, own_root, early = place(s, u)
            on = valid & ((y == yj) if first else (y < yj)) & ~done_early(s, u)
            arrived(on, quarter(zs.at[s, u], x), z_rsem.at[s, u, x])
            relay(s, u, on)

    def rest(s, u):
        on = needed(s, u, r) & ~done_early(s, u)
        for k in range(1, XS):
            q = lax.rem(x + k, XS)
            arrived(on, quarter(zs.at[s, u], q), z_rsem.at[s, u, q])

    def row_sends(s):
        for dz in (4, 3, 5, 2, 6, 1, 7):
            send(is_s[s], xr.at[s], xr.at[s], xr_ssem.at[s, dz - 1], xr_rsem.at[s],
                 (r, lax.rem(c + 2 * dz, cols)))

    def row_relay(s):
        solver = is_s[s]
        early = is_s[1] if s == 0 else jnp.bool_(False)
        mate = c + 1 - 2 * lax.rem(c, 2)
        to_early = (mate == sc[1]) if s == 0 else jnp.bool_(False)
        member = lax.rem(c, 2) == lax.rem(sc[s], 2)
        arrived(~solver & ~early, xr.at[s], xr_rsem.at[s])
        send(member & ~to_early, xr.at[s], xr.at[s], xr_ssem.at[s, 7], xr_rsem.at[s], (r, mate))

    def solve(s):
        for side in range(2):
            with jax.named_scope(f"wait_pq{s}{side}"):
                pltpu.make_async_copy(pq.at[s, side], pq.at[s, side], pq_rsem.at[s, side]).wait()
        pltpu.make_async_copy(el.at[s], el.at[s], e_rsem.at[s]).wait()
        left_e = jnp.transpose(el[s])[:, :1]
        right_e = ev[us[s]]
        mid = dot3(nn, pq[s, 0, 1], w[us[s]])
        mid = dot3(nt, mid, pq[s, 1, 1])
        mid = mid / (left_e + right_e)
        mid = dot3(nn, pq[s, 0, 0], mid)
        sol = -dot3(nt, mid, pq[s, 1, 0])
        hi, lo = split2(sol)
        xr[s, 0] = hi
        xr[s, 1] = lo
        if s == 0:
            zs[s, us[s], 0] = hi
            zs[s, us[s], 1] = lo
        else:
            last = r == rows - 1

            @pl.when(last)
            def _():
                th, tl = split2(jnp.transpose(sol))
                zs[s, us[s], 0] = th
                zs[s, us[s], 1] = tl

            @pl.when(~last)
            def _():
                zs[s, us[s], 0] = hi
                zs[s, us[s], 1] = lo

            @pl.when(~last & (c == tcol))
            def _():
                zs[s, tslot, 0] = hi
                zs[s, tslot, 1] = lo
        w[us[s]] = sol

    def terms(z, s, a, at, dot):
        return dot(a, z[0]) + dot(a, z[1]) + nn(xr[s, 0], at) + nn(xr[s, 1], at)

    u1 = us[1]
    with jax.named_scope("solve0"):
        pl.when(is_s[0])(functools.partial(solve, 0))
    early_sends()
    solver_sends(0)
    relay(0, us[0], is_s[0])
    row_sends(0)

    with jax.named_scope("early_wait_xr"):
        arrived(is_s[1], xr.at[0], xr_rsem.at[0])
    with jax.named_scope("early_wait_z"):
        early_on = is_s[1] & (r < rows - 1)
        for q in range(XS):
            arrived(early_on, quarter(zs.at[0, u1], q), z_rsem.at[0, u1, q])
        relay(0, u1, early_on)
    with jax.named_scope("early_wait_at"):
        arrived(is_s[1], at0.at[u1], at0_rsem.at[u1])

    @pl.when(is_s[1] & (r == rows - 1))
    def _():
        w[u1] = w[u1] - terms(xr.at[0], 0, a0[u1], at0[u1], nt)

    @pl.when(early_on)
    def _():
        w[u1] = w[u1] - terms(zs.at[0, u1], 0, a0[u1], at0[u1], nn)

    with jax.named_scope("solve1"):
        pl.when(is_s[1])(functools.partial(solve, 1))
    solver_sends(1)
    relay(1, u1, is_s[1])
    relay(1, tslot, is_s[1] & (c == tcol) & (r < rows - 1))
    row_sends(1)

    with jax.named_scope("at_forward"):
        for u in reversed(range(slots)):
            arrived(at_needed(r, u) & ~(is_s[1] & (u == u1)), at0.at[u], at0_rsem.at[u])
            send(at_needed(r, u) & (r >= 1), at0.at[u], at1.at[u], atf_ssem.at[u], at1_rsem.at[u],
                 (jnp.maximum(r - 1, 0), c))

    def update(s, a_ref, at_ref):
        for u in range(slots):
            m = c + cols * u
            target = (r <= m) & (r + m < nb - 1 - s)
            if s == 0:
                target = target & ~(is_s[1] & (u == u1))

            @pl.when(target)
            def _(u=u):
                w[u] = w[u] - terms(zs.at[s, u], s, a_ref[u], at_ref[u], nt if u < 2 else nn)

    with jax.named_scope("relay0a"):
        relays(0, True)
    with jax.named_scope("relay0b"):
        relays(0, False)
    with jax.named_scope("row0"):
        row_relay(0)
    with jax.named_scope("relay1a"):
        relays(1, True)
    with jax.named_scope("rest0"):
        for u in range(slots):
            rest(0, u)
    with jax.named_scope("update0"):
        update(0, a0, at0)
    with jax.named_scope("relay1b"):
        relays(1, False)
    with jax.named_scope("row1"):
        row_relay(1)
    with jax.named_scope("rest1"):
        for u in range(slots):
            rest(1, u)
    with jax.named_scope("wait_a1_at1"):
        for u in range(slots):
            need = step1_target(r, c + cols * u)
            arrived(need, a1.at[u], a1_rsem.at[u])
            arrived(at_needed(r + 1, u) & (r < rows - 1), at1.at[u], at1_rsem.at[u])
    with jax.named_scope("update1"):
        update(1, a1, at1)
    with jax.named_scope("write_out"):
        for u in range(slots):
            out[:, 0, u * BS:(u + 1) * BS] = w[u]
    with jax.named_scope("drain"):
        for pred, cp in pending:
            pl.when(pred)(cp.wait_send)


def solution(mesh):
    rows, cols = mesh.shape["row"], mesh.shape["col"]

    def on_device(state, coupling, coupling_t, factor, cofactor, rates):
        slots = 2 * rows // cols
        width = slots * BS
        any_space = pl.BlockSpec(memory_space=pl.ANY)
        vmem = pl.BlockSpec(memory_space=pltpu.VMEM)
        f32, bf16 = jnp.float32, jnp.bfloat16
        dma = pltpu.SemaphoreType.DMA
        return pl.pallas_call(
            functools.partial(kernel, rows, cols, slots),
            out_shape=jax.ShapeDtypeStruct((BS, 1, width), f32),
            in_specs=[any_space] * 6,
            out_specs=vmem,
            scratch_shapes=[
                pltpu.VMEM((BS, 1, width), f32),
                pltpu.VMEM((slots, BS, BS), f32),
                pltpu.VMEM((slots, BS, BS), bf16),
                pltpu.VMEM((slots, BS, BS), bf16),
                pltpu.VMEM((slots, BS, BS), bf16),
                pltpu.VMEM((slots, BS, BS), bf16),
                pltpu.VMEM((STEPS, 2, 2, BS, BS), f32),
                pltpu.VMEM((slots, 1, BS), f32),
                pltpu.VMEM((slots, 8, BS), f32),
                pltpu.VMEM((STEPS, 8, BS), f32),
                pltpu.VMEM((STEPS, 2, BS, BS), bf16),
                pltpu.VMEM((STEPS, slots, 2, BS, BS), bf16),
                dma((2 + slots,)),
                dma((STEPS, 2, 2, 2)),
                dma((STEPS, 2)),
                dma((STEPS,)),
                dma((STEPS,)),
                dma((slots,)),
                dma((slots,)),
                dma((slots,)),
                dma((slots,)),
                dma((slots,)),
                dma((slots,)),
                dma((STEPS, 8)),
                dma((STEPS,)),
                dma((STEPS, slots, rows // XS - 1 + XS - 1)),
                dma((STEPS, slots, XS)),
                dma((STEPS, 3 + XS)),
                dma((XS + 1,)),
            ],
            compiler_params=pltpu.CompilerParams(
                collective_id=0, has_side_effects=True, vmem_limit_bytes=63000 * 1024
            ),
        )(
            state,
            coupling.reshape(BS, width),
            coupling_t.reshape(2, BS, width),
            factor.reshape(slots, 8, BS),
            cofactor.reshape(slots, 8, BS),
            rates,
        )

    return jax.shard_map(
        on_device,
        mesh=mesh,
        in_specs=(
            P("row", "col", None),
            P("row", "col", None),
            P(None, "row", "col", None),
            P(None, "col", "row", None),
            P(None, "col", "row", None),
            P(None, "col", None),
        ),
        out_specs=P("row", "col", None),
        check_vma=False,
    )
```

```python
import functools

import jax
import jax.numpy as jnp
from jax import lax
from jax.experimental import pallas as pl
from jax.experimental.pallas import tpu as pltpu
from jax.sharding import PartitionSpec as P

MESH = pl.DeviceIdType.MESH
STEPS = 2
XS = 4
BS = 256


def split2(a):
    hi = a.astype(jnp.bfloat16)
    return hi, (a - hi.astype(jnp.float32)).astype(jnp.bfloat16)


QROWS = BS // XS
TOP = 32768.0


def bound(a):
    largest = jnp.max(jnp.max(jnp.abs(a), axis=0, keepdims=True), axis=1, keepdims=True)
    return (jnp.maximum(largest, 1e-30) * 1.01).astype(jnp.bfloat16).astype(jnp.float32)


def encode(a, top):
    v = a * (TOP / top)
    p = v * v
    p = p * p
    p = p * p
    return jnp.where(v < 0, -p, p).astype(jnp.bfloat16)


def decode(code, top):
    u = code.astype(jnp.float32)
    fourth = lax.rsqrt(lax.rsqrt(jnp.maximum(jnp.abs(u), 1.2e-38)))
    v = fourth * lax.rsqrt(fourth) * (top / TOP)
    return jnp.where(u < 0, -v, jnp.where(u > 0, v, 0.0))


def nn(a, b):
    return lax.dot_general(a, b, (((1,), (0,)), ((), ())), preferred_element_type=jnp.float32)


def nt(a, b):
    return lax.dot_general(a, b, (((1,), (1,)), ((), ())), preferred_element_type=jnp.float32)


def dot3(dot, a, b):
    ah, al = split2(a)
    bh, bl = split2(b)
    return dot(ah, bh) + dot(ah, bl) + dot(al, bh)


def kernel(
    rows, cols, slots,
    st_in, cp_in, ct_in, p_in, q_in, e_in, out,
    st, w, a0, a1, at0, at1, pq, own_pq, ev, es, el, xr, zs, xd, zd,
    loc_sem, pq_ssem, pq_rsem, e_ssem, e_rsem,
    at_ssem, at0_rsem, atf_ssem, at1_rsem, a1_ssem, a1_rsem,
    xr_ssem, xr_rsem, z_ssem, z_rsem, sv_ssem, er_ssem, fw_ssem, go_sem,
):
    r, c = lax.axis_index("row"), lax.axis_index("col")
    y, x = r // XS, lax.rem(r, XS)
    nb = 2 * rows
    pending = []

    def send(pred, src, dst, ssem, rsem, dev):
        cp = pltpu.make_async_remote_copy(
            src_ref=src, dst_ref=dst, send_sem=ssem, recv_sem=rsem,
            device_id=dev, device_id_type=MESH,
        )
        pl.when(pred)(cp.start)
        pending.append((pred, cp))

    def arrived(pred, dst, rsem):
        cp = pltpu.make_async_copy(dst, dst, rsem)
        pl.when(pred)(cp.wait)

    sc = [lax.rem(nb - 1 - s - r, cols) for s in range(STEPS)]
    us = [(nb - 1 - s - r) // cols for s in range(STEPS)]
    is_s = [c == sc[s] for s in range(STEPS)]
    tcol, tslot = lax.rem(r, cols), r // cols

    barrier = pltpu.get_barrier_semaphore()

    def greet(dr, dc):
        pl.semaphore_signal(barrier, inc=1, device_id=(dr, dc), device_id_type=MESH)

    ys = rows // XS
    for dx in range(1, XS):
        greet(y * XS + lax.rem(x + dx, XS), c)
    for dy in range(1, ys):
        greet(lax.rem(r + dy * XS, rows), c)
    greet(lax.rem(r + 1, rows), c)
    for dz in range(1, cols // 2):
        greet(r, lax.rem(c + 2 * dz, cols))
    greet(r, lax.rem(c + 1, cols))
    greet(r, c + 1 - 2 * lax.rem(c, 2))
    expected = XS - 1 + ys - 1 + 1 + cols // 2 - 1 + 2
    tj = y * XS + lax.rem(c, XS)
    near = lax.rem(y, cols // XS) == c // XS
    for s in range(STEPS):
        tj_col = lax.rem(nb - 1 - s - tj, cols)
        alone = (tj == r) & (tj_col == c)

        @pl.when(near & ~alone)
        def _(tj_col=tj_col):
            greet(tj, tj_col)

        expected = expected + jnp.where(is_s[s], XS, 0) - jnp.where(is_s[s] & (c == tcol), 1, 0)

        if s == 1:

            @pl.when(is_s[1] & (c != tcol))
            def _():
                greet(r, tcol)

            expected = expected + jnp.where((c == tcol) & (c != sc[1]), 1, 0)
            continue

        @pl.when(is_s[s])
        def _():
            for k in range(1, rows):
                greet(lax.rem(r + k, rows), c)

            for k in range(1, rows):
                greet(lax.rem(r + k, rows), tcol)

            @pl.when(c != tcol)
            def _():
                greet(r, tcol)

        expected = expected + 4 - jnp.where(is_s[s], 1, 0) - jnp.where(is_s[s] & (c == tcol), 1, 0)

    ld_st = pltpu.make_async_copy(st_in, st, loc_sem.at[0])
    ld_st.start()
    ld_a0 = [
        pltpu.make_async_copy(cp_in.at[:, pl.ds(u * BS, BS)], a0.at[u], loc_sem.at[1 + u])
        for u in range(slots)
    ]
    for cp in ld_a0:
        cp.start()
    ld_e = pltpu.make_async_copy(e_in, ev, loc_sem.at[1 + slots])
    ld_e.start()
    ld_pq = [
        pltpu.make_async_copy(ref, own_pq.at[:, t], loc_sem.at[2 + slots + t])
        for t, ref in enumerate((p_in, q_in))
    ]
    for cp in ld_pq:
        cp.start()
    ld_e.wait()
    for cp in ld_pq:
        cp.wait()
    es[...] = jnp.broadcast_to(ev[...], es.shape)
    with jax.named_scope("barrier"):
        pl.semaphore_wait(barrier, expected)

    def to_solver(side, q):
        slot = q + 2 * side
        m = c + cols * slot
        if side == 0:
            dr, dc = m, lax.rem(nb - 1 - m, cols)
        else:
            dr, dc = nb - 1 - m, c
        mine = (dr == r) & (dc == c)
        src = own_pq.at[slot]
        dst = pq.at[0, side, :, pl.ds(pl.multiple_of(r * 8, 8), 8), :]
        send(~mine, src, dst, pq_ssem.at[side, q], pq_rsem.at[0, side], (dr, dc))
        pl.when(mine)(pltpu.make_async_copy(src, dst, pq_rsem.at[0, side]).start)

    def rate_to_solver(s):
        have = c == tcol
        mine = c == sc[s]
        send(have & ~mine, es.at[tslot], el.at[s], e_ssem.at[s], e_rsem.at[s], (r, sc[s]))
        pl.when(have & mine)(pltpu.make_async_copy(es.at[tslot], el.at[s], e_rsem.at[s]).start)

    for side in range(2):
        for q in range(2):
            to_solver(side, q)
    for s in range(STEPS):
        rate_to_solver(s)

    def at_needed(g, u):
        m = c + cols * u
        return (m >= g - 1) & (m <= nb - 2 - g)

    g = lax.rem(r + rows // 2, rows)
    c_dn = lax.rem(c + cols - 1, cols)
    urgent = nb - 2 - g

    def step1_target(row, m):
        return (row <= m) & (row + m < nb - 2)

    def at_send(u, first):
        at_once = c + cols * u == urgent
        send(at_needed(g, u) & (at_once if first else ~at_once), ct_in.at[0, :, pl.ds(u * BS, BS)],
             at0.at[u], at_ssem.at[u], at0_rsem.at[u], (g, c))

    def bulk_sends():
        for u in reversed(range(slots)):
            at_send(u, False)
        for u in range(slots):
            wrap = jnp.where(c == 0, 1, 0)
            du = u - wrap
            send((du >= 0) & step1_target(r, c_dn + cols * du), cp_in.at[:, pl.ds(u * BS, BS)],
                 a1.at[jnp.maximum(du, 0)], a1_ssem.at[u], a1_rsem.at[jnp.maximum(du, 0)], (r, c_dn))

    with jax.named_scope("pq_sent"):
        for pred, cp in pending:
            pl.when(pred)(cp.wait_send)
        pending.clear()
        for dy in range(1, ys):
            pl.semaphore_signal(
                go_sem, inc=1, device_id=(lax.rem(r + dy * XS, rows), c), device_id_type=MESH
            )

    for u in range(1, slots):
        at_send(u, True)

    with jax.named_scope("local_in"):
        ld_st.wait()
        for u in range(slots):
            w[u] = st[:, 0, u * BS:(u + 1) * BS]
        for cp in ld_a0:
            cp.wait()

    def col_of(s, u):
        d = nb - 1 - s
        m = c + cols * u
        j = jnp.minimum(m, d - m)
        return d, m, j, m <= d

    def quarter(ref, q):
        return ref.at[q]

    def write_code(ref, a, top):
        code = encode(a, top)
        for q in range(XS):
            ref[q, :QROWS] = code[q * QROWS:(q + 1) * QROWS]
            ref[q, QROWS:] = jnp.broadcast_to(top, (8, BS)).astype(jnp.bfloat16)

    def read_code(ref, dst, order):
        for q in order:
            top = ref[q, QROWS:QROWS + 1, :].astype(jnp.float32)
            hi, lo = split2(decode(ref[q, :QROWS], top))
            dst[0, q * QROWS:(q + 1) * QROWS] = hi
            dst[1, q * QROWS:(q + 1) * QROWS] = lo

    def place(s, u):
        d = nb - 1 - s
        m = c + cols * u
        j = jnp.minimum(m, d - m)
        yj, xj = j // XS, lax.rem(j, XS)
        own_root = jnp.bool_(u >= 2) if isinstance(u, int) else u >= 2
        if s == 1:
            own_root = own_root | (lax.rem(j, cols // 2) == cols // 2 - 1)
        early = (j - 1) if s == 0 else j - 2 * rows
        early = jnp.where(u >= 2, early, -2 * rows)
        return j, yj, xj, m <= d, own_root, early

    def needed(s, u, row):
        j, yj, xj, valid, own_root, _ = place(s, u)
        return valid & ((row < j) | ((row == j) & ~own_root))

    def solver_sends(s):
        on = is_s[s]
        own = zs.at[s, us[s]]
        early = r - 1 if s == 0 else r - 2 * rows
        for k, dx in enumerate((3, 1, 2)):
            q = lax.rem(x + dx, XS)
            row = y * XS + q
            send(on & (row != early), quarter(own, q), quarter(own, q), sv_ssem.at[s, k],
                 z_rsem.at[s, us[s], q], (row, c))
        for q in range(XS):
            row = y * XS + q
            mine = (c == tcol) & (x == q)
            if s == 1:
                mine = mine | (r == rows - 1)
            send(on & ~mine, quarter(xr.at[s], q), quarter(zs.at[s, tslot], q), sv_ssem.at[s, 3 + q],
                 z_rsem.at[s, tslot, q], (row, tcol))

    def early_sends():
        on = is_s[0]
        send(on, xr.at[0], xr.at[0], er_ssem.at[XS], xr_rsem.at[0], (r, sc[1]))
        own = zs.at[0, us[0]]
        for q in range(XS):
            send(on & (r >= 1), quarter(own, q), quarter(own, q), er_ssem.at[q],
                 z_rsem.at[0, us[0], q], (jnp.maximum(r - 1, 0), c))

    def relay(s, u, on):
        j, yj, xj, valid, own_root, early = place(s, u)
        part = quarter(zs.at[s, u], x)
        first = on & valid & (y == yj)
        for y2 in range(ys - 1):
            row = y2 * XS + x
            send(first & (y2 < yj) & (row != early), part, part, z_ssem.at[s, u, y2],
                 z_rsem.at[s, u, x], (row, c))
        for k, dx in enumerate((1, 3, 2)):
            row = y * XS + lax.rem(x + dx, XS)
            send(on & needed(s, u, row) & (row != early), part, part, z_ssem.at[s, u, ys - 1 + k],
                 z_rsem.at[s, u, x], (row, c))

    def own_part(s, u):
        own = is_s[s] & (u == us[s])
        if s == 1:
            own = own | (is_s[s] & (c == tcol) & (u == tslot))
        return own

    def done_early(s, u):
        done = own_part(s, u)
        if s == 0:
            done = done | (is_s[1] & (u == u1) & (r < rows - 1))
        return done

    def relays(s, first):
        for u in (3, 0, 2, 1):
            j, yj, xj, valid, own_root, early = place(s, u)
            on = valid & ((y == yj) if first else (y < yj)) & ~done_early(s, u)
            arrived(on, quarter(zs.at[s, u], x), z_rsem.at[s, u, x])
            relay(s, u, on)

    def rest(s, u):
        on = needed(s, u, r) & ~done_early(s, u)
        for k in range(1, XS):
            q = lax.rem(x + k, XS)
            arrived(on, quarter(zs.at[s, u], q), z_rsem.at[s, u, q])

    def row_sends(s):
        for dz in (4, 3, 5, 2, 6, 1, 7):
            send(is_s[s], xr.at[s], xr.at[s], xr_ssem.at[s, dz - 1], xr_rsem.at[s],
                 (r, lax.rem(c + 2 * dz, cols)))

    def row_relay(s):
        solver = is_s[s]
        early = is_s[1] if s == 0 else jnp.bool_(False)
        mate = c + 1 - 2 * lax.rem(c, 2)
        to_early = (mate == sc[1]) if s == 0 else jnp.bool_(False)
        member = lax.rem(c, 2) == lax.rem(sc[s], 2)
        arrived(~solver & ~early, xr.at[s], xr_rsem.at[s])
        send(member & ~to_early, xr.at[s], xr.at[s], xr_ssem.at[s, 7], xr_rsem.at[s], (r, mate))

    def solve(s):
        right = jnp.where(r == rows - 1, 0, 1) if s == 1 else 1
        left_e = jnp.transpose(el[s])[:, :1]
        right_e = ev[us[s]]
        mid = dot3(nn, pq[s, 0, 1], w[us[s]])
        mid = dot3(nt, mid, pq[s, right, 1])
        mid = mid / (left_e + right_e)
        mid = dot3(nn, pq[s, 0, 0], mid)
        sol = -dot3(nt, mid, pq[s, right, 0])
        top = bound(sol)
        write_code(xr.at[s], sol, top)
        if s == 0:
            write_code(zs.at[s, us[s]], sol, top)
        else:
            last = r == rows - 1

            @pl.when(last)
            def _():
                write_code(zs.at[s, us[s]], jnp.transpose(sol), top)

            @pl.when(~last)
            def _():
                write_code(zs.at[s, us[s]], sol, top)

            @pl.when(~last & (c == tcol))
            def _():
                write_code(zs.at[s, tslot], sol, top)
        w[us[s]] = sol

    def terms(z, a, at, dot):
        return dot(a, z[0]) + dot(a, z[1]) + nn(xd[0], at) + nn(xd[1], at)

    u1 = us[1]
    def operators_ready(s):
        for side in range(2):
            on = is_s[s] & (r < rows - 1) if (s, side) == (1, 1) else is_s[s]
            arrived(on, pq.at[s, side], pq_rsem.at[s, side])
            if s == 0:
                to, dev = (on, (r, sc[1])) if side == 0 else (on & (r >= 1), (jnp.maximum(r - 1, 0), c))
                send(to, pq.at[0, side], pq.at[1, side], fw_ssem.at[side], pq_rsem.at[1, side], dev)
        arrived(is_s[s], el.at[s], e_rsem.at[s])

    with jax.named_scope("wait_pq00"):
        operators_ready(0)
    with jax.named_scope("solve0"):
        pl.when(is_s[0])(functools.partial(solve, 0))
    early_sends()
    solver_sends(0)
    relay(0, us[0], is_s[0])
    row_sends(0)
    with jax.named_scope("wait_go"):
        pl.semaphore_wait(go_sem, ys - 1)
    bulk_sends()

    with jax.named_scope("early_wait_xr"):
        arrived(is_s[1], xr.at[0], xr_rsem.at[0])
    with jax.named_scope("early_wait_z"):
        early_on = is_s[1] & (r < rows - 1)
        for q in range(XS):
            arrived(early_on, quarter(zs.at[0, u1], q), z_rsem.at[0, u1, q])
        relay(0, u1, early_on)
    with jax.named_scope("early_wait_at"):
        arrived(is_s[1], at0.at[u1], at0_rsem.at[u1])

    @pl.when(is_s[1])
    def _():
        read_code(xr.at[0], xd, range(XS))

    @pl.when(is_s[1] & (r == rows - 1))
    def _():
        w[u1] = w[u1] - terms(xd, a0[u1], at0[u1], nt)

    @pl.when(early_on)
    def _():
        read_code(zs.at[0, u1], zd, range(XS))
        w[u1] = w[u1] - terms(zd, a0[u1], at0[u1], nn)

    with jax.named_scope("wait_pq1"):
        operators_ready(1)
    with jax.named_scope("solve1"):
        pl.when(is_s[1])(functools.partial(solve, 1))
    solver_sends(1)
    relay(1, u1, is_s[1])
    relay(1, tslot, is_s[1] & (c == tcol) & (r < rows - 1))
    row_sends(1)

    def update(s, a_ref, at_ref):
        last_m = nb - 2 - s - r

        @pl.when(r <= last_m)
        def _():
            read_code(xr.at[s], xd, range(XS))

        for u in range(slots):
            m = c + cols * u
            target = (r <= m) & (m <= last_m)
            if s == 0:
                target = target & ~(is_s[1] & (u == u1))

            @pl.when(target)
            def _(u=u):
                read_code(zs.at[s, u], zd, range(XS))
                w[u] = w[u] - terms(zd, a_ref[u], at_ref[u], nt if u < 2 else nn)

    with jax.named_scope("relay0a"):
        relays(0, True)
    with jax.named_scope("relay1a"):
        relays(1, True)
    with jax.named_scope("relay0b"):
        relays(0, False)
    with jax.named_scope("at_forward"):
        for u in reversed(range(slots)):
            arrived(at_needed(r, u) & ~(is_s[1] & (u == u1)), at0.at[u], at0_rsem.at[u])
            send(at_needed(r, u) & (r >= 1), at0.at[u], at1.at[u], atf_ssem.at[u], at1_rsem.at[u],
                 (jnp.maximum(r - 1, 0), c))

    with jax.named_scope("relay1b"):
        relays(1, False)
    with jax.named_scope("row0"):
        row_relay(0)
    with jax.named_scope("row1"):
        row_relay(1)
    with jax.named_scope("rest0"):
        for u in range(slots):
            rest(0, u)
    with jax.named_scope("update0"):
        update(0, a0, at0)
    with jax.named_scope("wait_a1_at1"):
        for u in range(slots):
            need = step1_target(r, c + cols * u)
            arrived(need, a1.at[u], a1_rsem.at[u])
            arrived(at_needed(r + 1, u) & (r < rows - 1), at1.at[u], at1_rsem.at[u])
    with jax.named_scope("rest1"):
        for u in range(slots):
            rest(1, u)
    with jax.named_scope("update1"):
        update(1, a1, at1)
    with jax.named_scope("write_out"):
        for u in range(slots):
            out[:, 0, u * BS:(u + 1) * BS] = w[u]
    with jax.named_scope("drain"):
        for pred, cp in pending:
            pl.when(pred)(cp.wait_send)


def solution(mesh):
    rows, cols = mesh.shape["row"], mesh.shape["col"]

    def on_device(state, coupling, coupling_t, factor, cofactor, rates):
        slots = 2 * rows // cols
        width = slots * BS
        any_space = pl.BlockSpec(memory_space=pl.ANY)
        vmem = pl.BlockSpec(memory_space=pltpu.VMEM)
        f32, bf16 = jnp.float32, jnp.bfloat16
        dma = pltpu.SemaphoreType.DMA
        return pl.pallas_call(
            functools.partial(kernel, rows, cols, slots),
            out_shape=jax.ShapeDtypeStruct((BS, 1, width), f32),
            in_specs=[any_space] * 6,
            out_specs=vmem,
            scratch_shapes=[
                pltpu.VMEM((BS, 1, width), f32),
                pltpu.VMEM((slots, BS, BS), f32),
                pltpu.VMEM((slots, BS, BS), bf16),
                pltpu.VMEM((slots, BS, BS), bf16),
                pltpu.VMEM((slots, BS, BS), bf16),
                pltpu.VMEM((slots, BS, BS), bf16),
                pltpu.VMEM((STEPS, 2, 2, BS, BS), f32),
                pltpu.VMEM((slots, 2, 8, BS), f32),
                pltpu.VMEM((slots, 1, BS), f32),
                pltpu.VMEM((slots, 8, BS), f32),
                pltpu.VMEM((STEPS, 8, BS), f32),
                pltpu.VMEM((STEPS, XS, QROWS + 8, BS), bf16),
                pltpu.VMEM((STEPS, slots, XS, QROWS + 8, BS), bf16),
                pltpu.VMEM((2, BS, BS), bf16),
                pltpu.VMEM((2, BS, BS), bf16),
                dma((4 + slots,)),
                dma((2, 2)),
                dma((STEPS, 2)),
                dma((STEPS,)),
                dma((STEPS,)),
                dma((slots,)),
                dma((slots,)),
                dma((slots,)),
                dma((slots,)),
                dma((slots,)),
                dma((slots,)),
                dma((STEPS, 8)),
                dma((STEPS,)),
                dma((STEPS, slots, rows // XS - 1 + XS - 1)),
                dma((STEPS, slots, XS)),
                dma((STEPS, 3 + XS)),
                dma((XS + 1,)),
                dma((2,)),
                pltpu.SemaphoreType.REGULAR,
            ],
            compiler_params=pltpu.CompilerParams(
                collective_id=0, has_side_effects=True, vmem_limit_bytes=63000 * 1024
            ),
        )(
            state,
            coupling.reshape(BS, width),
            coupling_t.reshape(2, BS, width),
            factor.reshape(slots, 8, BS),
            cofactor.reshape(slots, 8, BS),
            rates,
        )

    return jax.shard_map(
        on_device,
        mesh=mesh,
        in_specs=(
            P("row", "col", None),
            P("row", "col", None),
            P(None, "row", "col", None),
            P(None, "col", "row", None),
            P(None, "col", "row", None),
            P(None, "col", None),
        ),
        out_specs=P("row", "col", None),
        check_vma=False,
    )
```

```python
import functools

import jax
import jax.numpy as jnp
from jax import lax
from jax.experimental import pallas as pl
from jax.experimental.pallas import tpu as pltpu
from jax.sharding import PartitionSpec as P

MESH = pl.DeviceIdType.MESH
STEPS = 2
XS = 4
BS = 256


def split2(a):
    hi = a.astype(jnp.bfloat16)
    return hi, (a - hi.astype(jnp.float32)).astype(jnp.bfloat16)


QROWS = BS // XS
TOP = 222.0


def bounds(a):
    largest = jnp.max(jnp.abs(a), axis=0, keepdims=True)
    return (jnp.maximum(largest, 1e-30) * 1.01).astype(jnp.bfloat16).astype(jnp.float32)


def encode(a, top):
    v = a * (TOP / top)
    p = v * v
    p = p * p
    p = p * p
    p = p * p
    return jnp.where(v < 0, -p, p).astype(jnp.bfloat16)


def decode(code, top):
    u = code.astype(jnp.float32)
    fourth = lax.rsqrt(lax.rsqrt(jnp.maximum(jnp.abs(u), 1.2e-38)))
    v = lax.rsqrt(lax.rsqrt(fourth)) * (top * (1.0 / TOP))
    return jnp.where(u < 0, -v, jnp.where(u > 0, v, 0.0))


def nn(a, b):
    return lax.dot_general(a, b, (((1,), (0,)), ((), ())), preferred_element_type=jnp.float32)


def nt(a, b):
    return lax.dot_general(a, b, (((1,), (1,)), ((), ())), preferred_element_type=jnp.float32)


def dot3(dot, a, b):
    ah, al = split2(a)
    bh, bl = split2(b)
    return dot(ah, bh) + dot(ah, bl) + dot(al, bh)


def kernel(
    rows, cols, slots,
    st_in, cp_in, ct_in, p_in, q_in, e_in, out,
    st, w, a0, a1, at0, at1, pq, own_pq, ev, es, el, xr, zs, xd, zd,
    loc_sem, pq_ssem, pq_rsem, e_ssem, e_rsem,
    at_ssem, at0_rsem, atf_ssem, at1_rsem, a1_ssem, a1_rsem,
    xr_ssem, xr_rsem, z_ssem, z_rsem, sv_ssem, er_ssem, fw_ssem, pq2_ssem, go_sem,
):
    r, c = lax.axis_index("row"), lax.axis_index("col")
    y, x = r // XS, lax.rem(r, XS)
    nb = 2 * rows
    pending = []

    def send(pred, src, dst, ssem, rsem, dev):
        cp = pltpu.make_async_remote_copy(
            src_ref=src, dst_ref=dst, send_sem=ssem, recv_sem=rsem,
            device_id=dev, device_id_type=MESH,
        )
        pl.when(pred)(cp.start)
        pending.append((pred, cp))

    def arrived(pred, dst, rsem):
        cp = pltpu.make_async_copy(dst, dst, rsem)
        pl.when(pred)(cp.wait)

    sc = [lax.rem(nb - 1 - s - r, cols) for s in range(STEPS)]
    us = [(nb - 1 - s - r) // cols for s in range(STEPS)]
    is_s = [c == sc[s] for s in range(STEPS)]
    tcol, tslot = lax.rem(r, cols), r // cols

    barrier = pltpu.get_barrier_semaphore()

    def greet(dr, dc):
        pl.semaphore_signal(barrier, inc=1, device_id=(dr, dc), device_id_type=MESH)

    ys = rows // XS
    for dx in range(1, XS):
        greet(y * XS + lax.rem(x + dx, XS), c)
    for dy in range(1, ys):
        greet(lax.rem(r + dy * XS, rows), c)
    greet(lax.rem(r + 1, rows), c)
    for dz in range(1, cols // 2):
        greet(r, lax.rem(c + 2 * dz, cols))
    greet(r, lax.rem(c + 1, cols))
    greet(r, c + 1 - 2 * lax.rem(c, 2))
    expected = XS - 1 + ys - 1 + 1 + cols // 2 - 1 + 2
    tj = y * XS + lax.rem(c, XS)
    near = lax.rem(y, cols // XS) == c // XS
    for s in range(STEPS):
        tj_col = lax.rem(nb - 1 - s - tj, cols)
        alone = (tj == r) & (tj_col == c)

        @pl.when(near & ~alone)
        def _(tj_col=tj_col):
            greet(tj, tj_col)

        expected = expected + jnp.where(is_s[s], XS, 0) - jnp.where(is_s[s] & (c == tcol), 1, 0)

        if s == 1:

            @pl.when(is_s[1] & (c != tcol))
            def _():
                greet(r, tcol)

            expected = expected + jnp.where((c == tcol) & (c != sc[1]), 1, 0)
            gathers = is_s[1] & (x == XS - 1) & (r < rows - 1)

            @pl.when(gathers)
            def _():
                for k in range(1, rows):
                    greet(lax.rem(r + k, rows), c)

            gatherers = jnp.where(c == cols - 1, 1, jnp.where(lax.rem(c, XS) == XS - 1, 2, 0))
            expected = expected + gatherers - jnp.where(gathers, 1, 0)
            continue

        @pl.when(is_s[s])
        def _():
            for k in range(1, rows):
                greet(lax.rem(r + k, rows), c)

            for k in range(1, rows):
                greet(lax.rem(r + k, rows), tcol)

            @pl.when(c != tcol)
            def _():
                greet(r, tcol)

        expected = expected + 4 - jnp.where(is_s[s], 1, 0) - jnp.where(is_s[s] & (c == tcol), 1, 0)

    ld_st = pltpu.make_async_copy(st_in, st, loc_sem.at[0])
    ld_st.start()
    ld_a0 = [
        pltpu.make_async_copy(cp_in.at[:, pl.ds(u * BS, BS)], a0.at[u], loc_sem.at[1 + u])
        for u in range(slots)
    ]
    for cp in ld_a0:
        cp.start()
    ld_e = pltpu.make_async_copy(e_in, ev, loc_sem.at[1 + slots])
    ld_e.start()
    ld_pq = [
        pltpu.make_async_copy(ref, own_pq.at[:, t], loc_sem.at[2 + slots + t])
        for t, ref in enumerate((p_in, q_in))
    ]
    for cp in ld_pq:
        cp.start()
    ld_e.wait()
    for cp in ld_pq:
        cp.wait()
    es[...] = jnp.broadcast_to(ev[...], es.shape)
    with jax.named_scope("barrier"):
        pl.semaphore_wait(barrier, expected)

    def to_solver(side, q):
        slot = q + 2 * side
        m = c + cols * slot
        if side == 0:
            dr, dc = m, lax.rem(nb - 1 - m, cols)
        else:
            dr, dc = nb - 1 - m, c
        mine = (dr == r) & (dc == c)
        src = own_pq.at[slot]
        dst = pq.at[0, side, :, pl.ds(pl.multiple_of(r * 8, 8), 8), :]
        send(~mine, src, dst, pq_ssem.at[side, q], pq_rsem.at[0, side], (dr, dc))
        pl.when(mine)(pltpu.make_async_copy(src, dst, pq_rsem.at[0, side]).start)

    def to_second_solver(q):
        m = c + cols * (2 + q)
        dr = nb - 2 - m
        on = (lax.rem(c, XS) == XS - 1) & (dr >= 0)
        mine = dr == r
        src = own_pq.at[2 + q]
        dst = pq.at[1, 1, :, pl.ds(pl.multiple_of(r * 8, 8), 8), :]
        send(on & ~mine, src, dst, pq2_ssem.at[q], pq_rsem.at[1, 1], (jnp.maximum(dr, 0), c))
        pl.when(on & mine)(pltpu.make_async_copy(src, dst, pq_rsem.at[1, 1]).start)

    def rate_to_solver(s):
        have = c == tcol
        mine = c == sc[s]
        send(have & ~mine, es.at[tslot], el.at[s], e_ssem.at[s], e_rsem.at[s], (r, sc[s]))
        pl.when(have & mine)(pltpu.make_async_copy(es.at[tslot], el.at[s], e_rsem.at[s]).start)

    for side in range(2):
        for q in range(2):
            to_solver(side, q)
    for q in range(2):
        to_second_solver(q)
    for s in range(STEPS):
        rate_to_solver(s)

    def at_needed(g, u):
        m = c + cols * u
        return (m >= g - 1) & (m <= nb - 2 - g)

    g = lax.rem(r + rows // 2, rows)
    c_dn = lax.rem(c + cols - 1, cols)
    urgent = nb - 2 - g

    def step1_target(row, m):
        return (row <= m) & (row + m < nb - 2)

    def at_send(u, first):
        at_once = c + cols * u == urgent
        send(at_needed(g, u) & (at_once if first else ~at_once), ct_in.at[0, :, pl.ds(u * BS, BS)],
             at0.at[u], at_ssem.at[u], at0_rsem.at[u], (g, c))

    def bulk_sends():
        for u in reversed(range(slots)):
            at_send(u, False)
        for u in range(slots):
            wrap = jnp.where(c == 0, 1, 0)
            du = u - wrap
            send((du >= 0) & step1_target(r, c_dn + cols * du), cp_in.at[:, pl.ds(u * BS, BS)],
                 a1.at[jnp.maximum(du, 0)], a1_ssem.at[u], a1_rsem.at[jnp.maximum(du, 0)], (r, c_dn))

    with jax.named_scope("pq_sent"):
        for pred, cp in pending:
            pl.when(pred)(cp.wait_send)
        pending.clear()
        for dy in range(1, ys):
            pl.semaphore_signal(
                go_sem, inc=1, device_id=(lax.rem(r + dy * XS, rows), c), device_id_type=MESH
            )

    for u in range(1, slots):
        at_send(u, True)

    with jax.named_scope("local_in"):
        ld_st.wait()
        for u in range(slots):
            w[u] = st[:, 0, u * BS:(u + 1) * BS]
        for cp in ld_a0:
            cp.wait()

    def col_of(s, u):
        d = nb - 1 - s
        m = c + cols * u
        j = jnp.minimum(m, d - m)
        return d, m, j, m <= d

    def quarter(ref, q):
        return ref.at[q]

    def write_code(a, *refs):
        for q in range(XS):
            part = a[q * QROWS:(q + 1) * QROWS]
            top = bounds(part)
            code = encode(part, top)
            tops = jnp.broadcast_to(top, (8, BS)).astype(jnp.bfloat16)
            for ref in refs:
                ref[q, :QROWS] = code
                ref[q, QROWS:] = tops

    def read_code(ref, dst, order):
        for q in order:
            top = ref[q, QROWS:QROWS + 1, :].astype(jnp.float32)
            hi, lo = split2(decode(ref[q, :QROWS], top))
            dst[0, q * QROWS:(q + 1) * QROWS] = hi
            dst[1, q * QROWS:(q + 1) * QROWS] = lo

    def place(s, u):
        d = nb - 1 - s
        m = c + cols * u
        j = jnp.minimum(m, d - m)
        yj, xj = j // XS, lax.rem(j, XS)
        own_root = jnp.bool_(u >= 2) if isinstance(u, int) else u >= 2
        if s == 1:
            own_root = own_root | (lax.rem(j, cols // 2) == cols // 2 - 1)
        early = (j - 1) if s == 0 else j - 2 * rows
        early = jnp.where(u >= 2, early, -2 * rows)
        return j, yj, xj, m <= d, own_root, early

    def needed(s, u, row):
        j, yj, xj, valid, own_root, _ = place(s, u)
        return valid & ((row < j) | ((row == j) & ~own_root))

    def solver_sends(s):
        on = is_s[s]
        own = zs.at[s, us[s]]
        early = r - 1 if s == 0 else r - 2 * rows
        for k, dx in enumerate((3, 1, 2)):
            q = lax.rem(x + dx, XS)
            row = y * XS + q
            send(on & (row != early), quarter(own, q), quarter(own, q), sv_ssem.at[s, k],
                 z_rsem.at[s, us[s], q], (row, c))
        for q in range(XS):
            row = y * XS + q
            mine = (c == tcol) & (x == q)
            if s == 1:
                mine = mine | (r == rows - 1)
            send(on & ~mine, quarter(xr.at[s], q), quarter(zs.at[s, tslot], q), sv_ssem.at[s, 3 + q],
                 z_rsem.at[s, tslot, q], (row, tcol))

    def early_sends():
        on = is_s[0]
        send(on, xr.at[0], xr.at[0], er_ssem.at[XS], xr_rsem.at[0], (r, sc[1]))
        own = zs.at[0, us[0]]
        for q in range(XS):
            send(on & (r >= 1), quarter(own, q), quarter(own, q), er_ssem.at[q],
                 z_rsem.at[0, us[0], q], (jnp.maximum(r - 1, 0), c))

    def relay(s, u, on):
        j, yj, xj, valid, own_root, early = place(s, u)
        part = quarter(zs.at[s, u], x)
        first = on & valid & (y == yj)
        for y2 in range(ys - 1):
            row = y2 * XS + x
            send(first & (y2 < yj) & (row != early), part, part, z_ssem.at[s, u, y2],
                 z_rsem.at[s, u, x], (row, c))
        for k, dx in enumerate((1, 3, 2)):
            row = y * XS + lax.rem(x + dx, XS)
            send(on & needed(s, u, row) & (row != early), part, part, z_ssem.at[s, u, ys - 1 + k],
                 z_rsem.at[s, u, x], (row, c))

    def own_part(s, u):
        own = is_s[s] & (u == us[s])
        if s == 1:
            own = own | (is_s[s] & (c == tcol) & (u == tslot))
        return own

    def done_early(s, u):
        done = own_part(s, u)
        if s == 0:
            done = done | (is_s[1] & (u == u1) & (r < rows - 1))
        return done

    def relays(s, first):
        for u in (3, 0, 2, 1):
            j, yj, xj, valid, own_root, early = place(s, u)
            on = valid & ((y == yj) if first else (y < yj)) & ~done_early(s, u)
            arrived(on, quarter(zs.at[s, u], x), z_rsem.at[s, u, x])
            relay(s, u, on)

    def rest(s, u):
        on = needed(s, u, r) & ~done_early(s, u)
        for k in range(1, XS):
            q = lax.rem(x + k, XS)
            arrived(on, quarter(zs.at[s, u], q), z_rsem.at[s, u, q])

    def row_sends(s):
        for dz in (4, 3, 5, 2, 6, 1, 7):
            send(is_s[s], xr.at[s], xr.at[s], xr_ssem.at[s, dz - 1], xr_rsem.at[s],
                 (r, lax.rem(c + 2 * dz, cols)))

    def row_relay(s):
        solver = is_s[s]
        early = is_s[1] if s == 0 else jnp.bool_(False)
        mate = c + 1 - 2 * lax.rem(c, 2)
        to_early = (mate == sc[1]) if s == 0 else jnp.bool_(False)
        member = lax.rem(c, 2) == lax.rem(sc[s], 2)
        arrived(~solver & ~early, xr.at[s], xr_rsem.at[s])
        send(member & ~to_early, xr.at[s], xr.at[s], xr_ssem.at[s, 7], xr_rsem.at[s], (r, mate))

    def solve(s):
        right = jnp.where(r == rows - 1, 0, 1) if s == 1 else 1
        left_e = jnp.transpose(el[s])[:, :1]
        right_e = ev[us[s]]
        mid = dot3(nn, pq[s, 0, 1], w[us[s]])
        mid = dot3(nt, mid, pq[s, right, 1])
        mid = mid / (left_e + right_e)
        mid = dot3(nn, pq[s, 0, 0], mid)
        sol = -dot3(nt, mid, pq[s, right, 0])
        if s == 0:
            write_code(sol, xr.at[s], zs.at[s, us[s]])
        else:
            write_code(sol, xr.at[s])
            last = r == rows - 1

            @pl.when(last)
            def _():
                write_code(jnp.transpose(sol), zs.at[s, us[s]])

            @pl.when(~last)
            def _():
                zs[s, us[s]] = xr[s]

            @pl.when(~last & (c == tcol))
            def _():
                zs[s, tslot] = xr[s]
        w[us[s]] = sol

    def terms(z, a, at, dot):
        return dot(a, z[0]) + dot(a, z[1]) + nn(xd[0], at) + nn(xd[1], at)

    u1 = us[1]
    def operators_ready(s):
        for side in range(2):
            on = is_s[s] & (r < rows - 1) if (s, side) == (1, 1) else is_s[s]
            arrived(on, pq.at[s, side], pq_rsem.at[s, side])
            if s == 0:
                to, dev = (on, (r, sc[1])) if side == 0 else (on & (x >= 1), (jnp.maximum(r - 1, 0), c))
                send(to, pq.at[0, side], pq.at[1, side], fw_ssem.at[side], pq_rsem.at[1, side], dev)
        arrived(is_s[s], el.at[s], e_rsem.at[s])

    with jax.named_scope("wait_pq00"):
        operators_ready(0)
    with jax.named_scope("solve0"):
        pl.when(is_s[0])(functools.partial(solve, 0))
    early_sends()
    solver_sends(0)
    relay(0, us[0], is_s[0])
    row_sends(0)
    with jax.named_scope("wait_go"):
        pl.semaphore_wait(go_sem, ys - 1)
    bulk_sends()

    with jax.named_scope("early_wait_xr"):
        arrived(is_s[1], xr.at[0], xr_rsem.at[0])
    with jax.named_scope("early_wait_z"):
        early_on = is_s[1] & (r < rows - 1)
        for q in range(XS):
            arrived(early_on, quarter(zs.at[0, u1], q), z_rsem.at[0, u1, q])
        relay(0, u1, early_on)
    with jax.named_scope("early_wait_at"):
        arrived(is_s[1], at0.at[u1], at0_rsem.at[u1])

    @pl.when(is_s[1])
    def _():
        read_code(xr.at[0], xd, range(XS))

    @pl.when(is_s[1] & (r == rows - 1))
    def _():
        w[u1] = w[u1] - terms(xd, a0[u1], at0[u1], nt)

    @pl.when(early_on)
    def _():
        read_code(zs.at[0, u1], zd, range(XS))
        w[u1] = w[u1] - terms(zd, a0[u1], at0[u1], nn)

    with jax.named_scope("wait_pq1"):
        operators_ready(1)
    with jax.named_scope("solve1"):
        pl.when(is_s[1])(functools.partial(solve, 1))
    solver_sends(1)
    relay(1, u1, is_s[1])
    relay(1, tslot, is_s[1] & (c == tcol) & (r < rows - 1))
    row_sends(1)

    def at_forward(u):
        with jax.named_scope(f"at_forward{u}"):
            arrived(at_needed(r, u) & ~(is_s[1] & (u == u1)), at0.at[u], at0_rsem.at[u])
            send(at_needed(r, u) & (r >= 1), at0.at[u], at1.at[u], atf_ssem.at[u], at1_rsem.at[u],
                 (jnp.maximum(r - 1, 0), c))

    at_forward(3)
    with jax.named_scope("relay0a"):
        relays(0, True)
    at_forward(2)
    with jax.named_scope("relay1a"):
        relays(1, True)
    at_forward(1)
    with jax.named_scope("relay0b"):
        relays(0, False)
    at_forward(0)
    with jax.named_scope("relay1b"):
        relays(1, False)
    with jax.named_scope("row0"):
        row_relay(0)
    with jax.named_scope("row1"):
        row_relay(1)
    def update(s, a_ref, at_ref):
        last_m = nb - 2 - s - r

        @pl.when(r <= last_m)
        def _():
            read_code(xr.at[s], xd, range(XS))

        for u in (3, 0, 2, 1):
            m = c + cols * u
            target = (r <= m) & (m <= last_m)
            if s == 0:
                target = target & ~(is_s[1] & (u == u1))
            with jax.named_scope(f"rest{s}_{u}"):
                rest(s, u)

            @pl.when(target)
            def _(u=u):
                read_code(zs.at[s, u], zd, range(XS))
                w[u] = w[u] - terms(zd, a_ref[u], at_ref[u], nt if u < 2 else nn)

            if s == 1:
                out[:, 0, u * BS:(u + 1) * BS] = w[u]

    with jax.named_scope("update0"):
        update(0, a0, at0)
    with jax.named_scope("wait_a1_at1"):
        for u in range(slots):
            need = step1_target(r, c + cols * u)
            arrived(need, a1.at[u], a1_rsem.at[u])
            arrived(at_needed(r + 1, u) & (r < rows - 1), at1.at[u], at1_rsem.at[u])
    with jax.named_scope("drain"):
        for pred, cp in pending:
            pl.when(pred)(cp.wait_send)
    with jax.named_scope("update1"):
        update(1, a1, at1)


def solution(mesh):
    rows, cols = mesh.shape["row"], mesh.shape["col"]

    def on_device(state, coupling, coupling_t, factor, cofactor, rates):
        slots = 2 * rows // cols
        width = slots * BS
        hbm = pl.BlockSpec(memory_space=pltpu.HBM)
        vmem = pl.BlockSpec(memory_space=pltpu.VMEM)
        f32, bf16 = jnp.float32, jnp.bfloat16
        dma = pltpu.SemaphoreType.DMA
        return pl.pallas_call(
            functools.partial(kernel, rows, cols, slots),
            out_shape=pltpu.VMEM((BS, 1, width), f32),
            in_specs=[hbm] * 6,
            out_specs=vmem,
            scratch_shapes=[
                pltpu.VMEM((BS, 1, width), f32),
                pltpu.VMEM((slots, BS, BS), f32),
                pltpu.VMEM((slots, BS, BS), bf16),
                pltpu.VMEM((slots, BS, BS), bf16),
                pltpu.VMEM((slots, BS, BS), bf16),
                pltpu.VMEM((slots, BS, BS), bf16),
                pltpu.VMEM((STEPS, 2, 2, BS, BS), f32),
                pltpu.VMEM((slots, 2, 8, BS), f32),
                pltpu.VMEM((slots, 1, BS), f32),
                pltpu.VMEM((slots, 8, BS), f32),
                pltpu.VMEM((STEPS, 8, BS), f32),
                pltpu.VMEM((STEPS, XS, QROWS + 8, BS), bf16),
                pltpu.VMEM((STEPS, slots, XS, QROWS + 8, BS), bf16),
                pltpu.VMEM((2, BS, BS), bf16),
                pltpu.VMEM((2, BS, BS), bf16),
                dma((4 + slots,)),
                dma((2, 2)),
                dma((STEPS, 2)),
                dma((STEPS,)),
                dma((STEPS,)),
                dma((slots,)),
                dma((slots,)),
                dma((slots,)),
                dma((slots,)),
                dma((slots,)),
                dma((slots,)),
                dma((STEPS, 8)),
                dma((STEPS,)),
                dma((STEPS, slots, rows // XS - 1 + XS - 1)),
                dma((STEPS, slots, XS)),
                dma((STEPS, 3 + XS)),
                dma((XS + 1,)),
                dma((2,)),
                dma((2,)),
                pltpu.SemaphoreType.REGULAR,
            ],
            compiler_params=pltpu.CompilerParams(
                collective_id=0, has_side_effects=True, vmem_limit_bytes=60000 * 1024
            ),
        )(
            state,
            coupling.reshape(BS, width),
            coupling_t.reshape(2, BS, width),
            factor.reshape(slots, 8, BS),
            cofactor.reshape(slots, 8, BS),
            rates,
        )

    return jax.shard_map(
        on_device,
        mesh=mesh,
        in_specs=(
            P("row", "col", None),
            P("row", "col", None),
            P(None, "row", "col", None),
            P(None, "col", "row", None),
            P(None, "col", "row", None),
            P(None, "col", None),
        ),
        out_specs=P("row", "col", None),
        check_vma=False,
    )
```

```python
import functools

import jax
import jax.numpy as jnp
from jax import lax
from jax.experimental import pallas as pl
from jax.experimental.pallas import tpu as pltpu
from jax.sharding import PartitionSpec as P

MESH = pl.DeviceIdType.MESH
STEPS = 2
XS = 4
BS = 256


def split2(a):
    hi = a.astype(jnp.bfloat16)
    return hi, (a - hi.astype(jnp.float32)).astype(jnp.bfloat16)


QROWS = BS // XS
TOP = 222.0


def bounds(a):
    largest = jnp.max(jnp.abs(a), axis=0, keepdims=True)
    return (jnp.maximum(largest, 1e-30) * 1.01).astype(jnp.bfloat16).astype(jnp.float32)


def encode(a, top):
    v = a * (TOP / top)
    p = v * v
    p = p * p
    p = p * p
    p = p * p
    return jnp.where(v < 0, -p, p).astype(jnp.bfloat16)


def decode(code, top):
    u = code.astype(jnp.float32)
    fourth = lax.rsqrt(lax.rsqrt(jnp.maximum(jnp.abs(u), 1.2e-38)))
    v = lax.rsqrt(lax.rsqrt(fourth)) * (top * (1.0 / TOP))
    return jnp.where(u < 0, -v, jnp.where(u > 0, v, 0.0))


def nn(a, b):
    return lax.dot_general(a, b, (((1,), (0,)), ((), ())), preferred_element_type=jnp.float32)


def nt(a, b):
    return lax.dot_general(a, b, (((1,), (1,)), ((), ())), preferred_element_type=jnp.float32)


def dot3(dot, a, b):
    ah, al = split2(a)
    bh, bl = split2(b)
    return dot(ah, bh) + dot(ah, bl) + dot(al, bh)


def kernel(
    rows, cols, slots,
    st_in, cp_in, ct_in, p_in, q_in, e_in, out,
    st, w, a0, a1, at0, at1, pq, own_pq, ev, es, el, xr, zs, xd, zd,
    loc_sem, pq_ssem, pq_rsem, e_ssem, e_rsem,
    at_ssem, at0_rsem, atf_ssem, at1_rsem, a1_ssem, a1_rsem,
    xr_ssem, xr_rsem, z_ssem, z_rsem, sv_ssem, er_ssem, fw_ssem, pq2_ssem, go_sem,
):
    r, c = lax.axis_index("row"), lax.axis_index("col")
    y, x = r // XS, lax.rem(r, XS)
    nb = 2 * rows
    pending = []

    def send(pred, src, dst, ssem, rsem, dev):
        cp = pltpu.make_async_remote_copy(
            src_ref=src, dst_ref=dst, send_sem=ssem, recv_sem=rsem,
            device_id=dev, device_id_type=MESH,
        )
        pl.when(pred)(cp.start)
        pending.append((pred, cp))

    def arrived(pred, dst, rsem):
        cp = pltpu.make_async_copy(dst, dst, rsem)
        pl.when(pred)(cp.wait)

    sc = [lax.rem(nb - 1 - s - r, cols) for s in range(STEPS)]
    us = [(nb - 1 - s - r) // cols for s in range(STEPS)]
    is_s = [c == sc[s] for s in range(STEPS)]
    tcol, tslot = lax.rem(r, cols), r // cols

    barrier = pltpu.get_barrier_semaphore()

    def greet(dr, dc):
        pl.semaphore_signal(barrier, inc=1, device_id=(dr, dc), device_id_type=MESH)

    ys = rows // XS
    for dx in range(1, XS):
        greet(y * XS + lax.rem(x + dx, XS), c)
    for dy in range(1, ys):
        greet(lax.rem(r + dy * XS, rows), c)
    greet(lax.rem(r + 1, rows), c)
    for dz in range(1, cols // 2):
        greet(r, lax.rem(c + 2 * dz, cols))
    greet(r, lax.rem(c + 1, cols))
    greet(r, c + 1 - 2 * lax.rem(c, 2))
    expected = XS - 1 + ys - 1 + 1 + cols // 2 - 1 + 2
    tj = y * XS + lax.rem(c, XS)
    near = lax.rem(y, cols // XS) == c // XS
    for s in range(STEPS):
        tj_col = lax.rem(nb - 1 - s - tj, cols)
        alone = (tj == r) & (tj_col == c)

        @pl.when(near & ~alone)
        def _(tj_col=tj_col):
            greet(tj, tj_col)

        expected = expected + jnp.where(is_s[s], XS, 0) - jnp.where(is_s[s] & (c == tcol), 1, 0)

        if s == 1:

            @pl.when(is_s[1] & (c != tcol))
            def _():
                greet(r, tcol)

            expected = expected + jnp.where((c == tcol) & (c != sc[1]), 1, 0)
            gathers = is_s[1] & (x == XS - 1) & (r < rows - 1)

            @pl.when(gathers)
            def _():
                for k in range(1, rows):
                    greet(lax.rem(r + k, rows), c)

            gatherers = jnp.where(c == cols - 1, 1, jnp.where(lax.rem(c, XS) == XS - 1, 2, 0))
            expected = expected + gatherers - jnp.where(gathers, 1, 0)
            continue

        @pl.when(is_s[s])
        def _():
            for k in range(1, rows):
                greet(lax.rem(r + k, rows), c)

            for k in range(1, rows):
                greet(lax.rem(r + k, rows), tcol)

            @pl.when(c != tcol)
            def _():
                greet(r, tcol)

        expected = expected + 4 - jnp.where(is_s[s], 1, 0) - jnp.where(is_s[s] & (c == tcol), 1, 0)

    ld_st = pltpu.make_async_copy(st_in, st, loc_sem.at[0])
    ld_st.start()
    ld_a0 = [
        pltpu.make_async_copy(cp_in.at[:, pl.ds(u * BS, BS)], a0.at[u], loc_sem.at[1 + u])
        for u in range(slots)
    ]
    for cp in ld_a0:
        cp.start()
    ld_e = pltpu.make_async_copy(e_in, ev, loc_sem.at[1 + slots])
    ld_e.start()
    ld_pq = [
        pltpu.make_async_copy(ref, own_pq.at[:, t], loc_sem.at[2 + slots + t])
        for t, ref in enumerate((p_in, q_in))
    ]
    for cp in ld_pq:
        cp.start()
    ld_e.wait()
    for cp in ld_pq:
        cp.wait()
    es[...] = jnp.broadcast_to(ev[...], es.shape)
    with jax.named_scope("barrier"):
        pl.semaphore_wait(barrier, expected)

    def to_solver(side, q):
        slot = q + 2 * side
        m = c + cols * slot
        if side == 0:
            dr, dc = m, lax.rem(nb - 1 - m, cols)
        else:
            dr, dc = nb - 1 - m, c
        mine = (dr == r) & (dc == c)
        src = own_pq.at[slot]
        dst = pq.at[0, side, :, pl.ds(pl.multiple_of(r * 8, 8), 8), :]
        send(~mine, src, dst, pq_ssem.at[side, q], pq_rsem.at[0, side], (dr, dc))
        pl.when(mine)(pltpu.make_async_copy(src, dst, pq_rsem.at[0, side]).start)

    def to_second_solver(q):
        m = c + cols * (2 + q)
        dr = nb - 2 - m
        on = (lax.rem(c, XS) == XS - 1) & (dr >= 0)
        mine = dr == r
        src = own_pq.at[2 + q]
        dst = pq.at[1, 1, :, pl.ds(pl.multiple_of(r * 8, 8), 8), :]
        send(on & ~mine, src, dst, pq2_ssem.at[q], pq_rsem.at[1, 1], (jnp.maximum(dr, 0), c))
        pl.when(on & mine)(pltpu.make_async_copy(src, dst, pq_rsem.at[1, 1]).start)

    def rate_to_solver(s):
        have = c == tcol
        mine = c == sc[s]
        send(have & ~mine, es.at[tslot], el.at[s], e_ssem.at[s], e_rsem.at[s], (r, sc[s]))
        pl.when(have & mine)(pltpu.make_async_copy(es.at[tslot], el.at[s], e_rsem.at[s]).start)

    for q in range(2):
        to_solver(0, q)
    in_plane = len(pending)
    for q in range(2):
        to_solver(1, q)
    for q in range(2):
        to_second_solver(q)
    for s in range(STEPS):
        rate_to_solver(s)

    def at_needed(g, u):
        m = c + cols * u
        return (m >= g - 1) & (m <= nb - 2 - g)

    g = lax.rem(r + rows // 2, rows)
    c_dn = lax.rem(c + cols - 1, cols)
    urgent = nb - 2 - g

    def step1_target(row, m):
        return (row <= m) & (row + m < nb - 2)

    def at_send(u, first):
        at_once = c + cols * u == urgent
        send(at_needed(g, u) & (at_once if first else ~at_once), ct_in.at[0, :, pl.ds(u * BS, BS)],
             at0.at[u], at_ssem.at[u], at0_rsem.at[u], (g, c))

    def bulk_sends():
        for u in reversed(range(slots)):
            at_send(u, False)
        for u in range(slots):
            wrap = jnp.where(c == 0, 1, 0)
            du = u - wrap
            send((du >= 0) & step1_target(r, c_dn + cols * du), cp_in.at[:, pl.ds(u * BS, BS)],
                 a1.at[jnp.maximum(du, 0)], a1_ssem.at[u], a1_rsem.at[jnp.maximum(du, 0)], (r, c_dn))

    with jax.named_scope("pq_sent"):
        for dy in range(1, ys):
            pl.semaphore_signal(
                go_sem, inc=1, device_id=(lax.rem(r + dy * XS, rows), c), device_id_type=MESH
            )

    for u in range(1, slots):
        at_send(u, True)

    with jax.named_scope("local_in"):
        ld_st.wait()
        for u in range(slots):
            w[u] = st[:, 0, u * BS:(u + 1) * BS]
        for cp in ld_a0:
            cp.wait()

    def col_of(s, u):
        d = nb - 1 - s
        m = c + cols * u
        j = jnp.minimum(m, d - m)
        return d, m, j, m <= d

    def quarter(ref, q):
        return ref.at[q]

    def write_code(a, *refs):
        for q in range(XS):
            part = a[q * QROWS:(q + 1) * QROWS]
            top = bounds(part)
            code = encode(part, top)
            tops = jnp.broadcast_to(top, (8, BS)).astype(jnp.bfloat16)
            for ref in refs:
                ref[q, :QROWS] = code
                ref[q, QROWS:] = tops

    def read_code(ref, dst, order):
        for q in order:
            top = ref[q, QROWS:QROWS + 1, :].astype(jnp.float32)
            hi, lo = split2(decode(ref[q, :QROWS], top))
            dst[0, q * QROWS:(q + 1) * QROWS] = hi
            dst[1, q * QROWS:(q + 1) * QROWS] = lo

    def place(s, u):
        d = nb - 1 - s
        m = c + cols * u
        j = jnp.minimum(m, d - m)
        yj, xj = j // XS, lax.rem(j, XS)
        own_root = jnp.bool_(u >= 2) if isinstance(u, int) else u >= 2
        if s == 1:
            own_root = own_root | (lax.rem(j, cols // 2) == cols // 2 - 1)
        early = (j - 1) if s == 0 else j - 2 * rows
        early = jnp.where(u >= 2, early, -2 * rows)
        return j, yj, xj, m <= d, own_root, early

    def needed(s, u, row):
        j, yj, xj, valid, own_root, _ = place(s, u)
        return valid & ((row < j) | ((row == j) & ~own_root))

    def solver_sends(s):
        on = is_s[s]
        own = zs.at[s, us[s]]
        early = r - 1 if s == 0 else r - 2 * rows
        for k, dx in enumerate((3, 1, 2)):
            q = lax.rem(x + dx, XS)
            row = y * XS + q
            send(on & (row != early), quarter(own, q), quarter(own, q), sv_ssem.at[s, k],
                 z_rsem.at[s, us[s], q], (row, c))
        for q in range(XS):
            row = y * XS + q
            mine = (c == tcol) & (x == q)
            if s == 1:
                mine = mine | (r == rows - 1)
            send(on & ~mine, quarter(xr.at[s], q), quarter(zs.at[s, tslot], q), sv_ssem.at[s, 3 + q],
                 z_rsem.at[s, tslot, q], (row, tcol))

    def early_sends():
        on = is_s[0]
        send(on, xr.at[0], xr.at[0], er_ssem.at[XS], xr_rsem.at[0], (r, sc[1]))
        own = zs.at[0, us[0]]
        for q in range(XS):
            send(on & (r >= 1), quarter(own, q), quarter(own, q), er_ssem.at[q],
                 z_rsem.at[0, us[0], q], (jnp.maximum(r - 1, 0), c))

    def relay(s, u, on):
        j, yj, xj, valid, own_root, early = place(s, u)
        part = quarter(zs.at[s, u], x)
        first = on & valid & (y == yj)
        for y2 in range(ys - 1):
            row = y2 * XS + x
            send(first & (y2 < yj) & (row != early), part, part, z_ssem.at[s, u, y2],
                 z_rsem.at[s, u, x], (row, c))
        for k, dx in enumerate((1, 3, 2)):
            row = y * XS + lax.rem(x + dx, XS)
            send(on & needed(s, u, row) & (row != early), part, part, z_ssem.at[s, u, ys - 1 + k],
                 z_rsem.at[s, u, x], (row, c))

    def own_part(s, u):
        own = is_s[s] & (u == us[s])
        if s == 1:
            own = own | (is_s[s] & (c == tcol) & (u == tslot))
        return own

    def done_early(s, u):
        done = own_part(s, u)
        if s == 0:
            done = done | (is_s[1] & (u == u1) & (r < rows - 1))
        return done

    def relays(s, first, part=(3, 0, 2, 1)):
        for u in part:
            j, yj, xj, valid, own_root, early = place(s, u)
            on = valid & ((y == yj) if first else (y < yj)) & ~done_early(s, u)
            arrived(on, quarter(zs.at[s, u], x), z_rsem.at[s, u, x])
            relay(s, u, on)

    def rest(s, u):
        on = needed(s, u, r) & ~done_early(s, u)
        for k in range(1, XS):
            q = lax.rem(x + k, XS)
            arrived(on, quarter(zs.at[s, u], q), z_rsem.at[s, u, q])

    def row_sends(s):
        for dz in (4, 3, 5, 2, 6, 1, 7):
            send(is_s[s], xr.at[s], xr.at[s], xr_ssem.at[s, dz - 1], xr_rsem.at[s],
                 (r, lax.rem(c + 2 * dz, cols)))

    def row_relay(s):
        solver = is_s[s]
        early = is_s[1] if s == 0 else jnp.bool_(False)
        mate = c + 1 - 2 * lax.rem(c, 2)
        to_early = (mate == sc[1]) if s == 0 else jnp.bool_(False)
        member = lax.rem(c, 2) == lax.rem(sc[s], 2)
        arrived(~solver & ~early, xr.at[s], xr_rsem.at[s])
        send(member & ~to_early, xr.at[s], xr.at[s], xr_ssem.at[s, 7], xr_rsem.at[s], (r, mate))

    def solve(s):
        right = jnp.where(r == rows - 1, 0, 1) if s == 1 else 1
        left_e = jnp.transpose(el[s])[:, :1]
        right_e = ev[us[s]]
        mid = dot3(nn, pq[s, 0, 1], w[us[s]])
        mid = dot3(nt, mid, pq[s, right, 1])
        mid = mid / (left_e + right_e)
        mid = dot3(nn, pq[s, 0, 0], mid)
        sol = -dot3(nt, mid, pq[s, right, 0])
        if s == 0:
            write_code(sol, xr.at[s], zs.at[s, us[s]])
        else:
            write_code(sol, xr.at[s])
            last = r == rows - 1

            @pl.when(last)
            def _():
                write_code(jnp.transpose(sol), zs.at[s, us[s]])

            @pl.when(~last)
            def _():
                zs[s, us[s]] = xr[s]

            @pl.when(~last & (c == tcol))
            def _():
                zs[s, tslot] = xr[s]
        w[us[s]] = sol

    def terms(z, x_row, a, at, dot):
        return dot(a, z[0]) + dot(a, z[1]) + nn(x_row[0], at) + nn(x_row[1], at)

    u1 = us[1]
    def operators_ready(s):
        for side in range(2):
            on = is_s[s] & (r < rows - 1) if (s, side) == (1, 1) else is_s[s]
            arrived(on, pq.at[s, side], pq_rsem.at[s, side])
            if s == 0:
                to, dev = (on, (r, sc[1])) if side == 0 else (on & (x >= 1), (jnp.maximum(r - 1, 0), c))
                send(to, pq.at[0, side], pq.at[1, side], fw_ssem.at[side], pq_rsem.at[1, side], dev)
        arrived(is_s[s], el.at[s], e_rsem.at[s])

    with jax.named_scope("wait_pq00"):
        operators_ready(0)
    with jax.named_scope("solve0"):
        pl.when(is_s[0])(functools.partial(solve, 0))
    early_sends()
    solver_sends(0)
    relay(0, us[0], is_s[0])
    row_sends(0)
    with jax.named_scope("wait_go"):
        pl.semaphore_wait(go_sem, ys - 1)
    bulk_sends()

    with jax.named_scope("early_wait_xr"):
        arrived(is_s[1], xr.at[0], xr_rsem.at[0])
    with jax.named_scope("early_wait_z"):
        early_on = is_s[1] & (r < rows - 1)
        for q in range(XS):
            arrived(early_on, quarter(zs.at[0, u1], q), z_rsem.at[0, u1, q])
        relay(0, u1, early_on)
    with jax.named_scope("early_wait_at"):
        arrived(is_s[1], at0.at[u1], at0_rsem.at[u1])

    @pl.when(is_s[1])
    def _():
        read_code(xr.at[0], xd.at[0], range(XS))

    @pl.when(is_s[1] & (r == rows - 1))
    def _():
        w[u1] = w[u1] - terms(xd.at[0], xd.at[0], a0[u1], at0[u1], nt)

    @pl.when(early_on)
    def _():
        read_code(zs.at[0, u1], zd, range(XS))
        w[u1] = w[u1] - terms(zd, xd.at[0], a0[u1], at0[u1], nn)

    with jax.named_scope("wait_pq1"):
        operators_ready(1)
    with jax.named_scope("solve1"):
        pl.when(is_s[1])(functools.partial(solve, 1))
    solver_sends(1)
    relay(1, u1, is_s[1])
    relay(1, tslot, is_s[1] & (c == tcol) & (r < rows - 1))
    row_sends(1)

    def at_forward(u):
        with jax.named_scope(f"at_forward{u}"):
            arrived(at_needed(r, u) & ~(is_s[1] & (u == u1)), at0.at[u], at0_rsem.at[u])
            send(at_needed(r, u) & (r >= 1), at0.at[u], at1.at[u], atf_ssem.at[u], at1_rsem.at[u],
                 (jnp.maximum(r - 1, 0), c))

    def step(name, *args):
        with jax.named_scope(name):
            relays(*args)

    at_forward(3)
    step("relay0a", 0, True)
    at_forward(2)
    step("relay0b_3", 0, False, (3,))
    step("relay0b_0", 0, False, (0,))
    step("relay1a", 1, True)
    sent_early = len(pending)
    at_forward(1)
    at_forward(0)
    step("relay0b_2", 0, False, (2,))
    step("relay0b_1", 0, False, (1,))
    step("relay1b_3", 1, False, (3,))
    step("relay1b_0", 1, False, (0,))
    step("relay1b_2", 1, False, (2,))
    step("relay1b_1", 1, False, (1,))
    with jax.named_scope("row0"):
        row_relay(0)
    with jax.named_scope("row1"):
        row_relay(1)
    def read_row(s):
        @pl.when(r <= nb - 2 - s - r)
        def _():
            read_code(xr.at[s], xd.at[s], range(XS))

    def update(s, a_ref, at_ref):
        for u in (3, 2, 0, 1) if s == 1 else (3, 0, 2, 1):
            m = c + cols * u
            target = (r <= m) & (r + m < nb - 1 - s)
            if s == 0:
                target = target & ~(is_s[1] & (u == u1))
            with jax.named_scope(f"rest{s}_{u}"):
                rest(s, u)
            if s == 1:
                with jax.named_scope(f"wait_at1_{u}"):
                    arrived(step1_target(r, m), a1.at[u], a1_rsem.at[u])
                    arrived(at_needed(r + 1, u) & (r < rows - 1), at1.at[u], at1_rsem.at[u])

            @pl.when(target)
            def _(u=u):
                read_code(zs.at[s, u], zd, range(XS))
                w[u] = w[u] - terms(zd, xd.at[s], a_ref[u], at_ref[u], nt if u < 2 else nn)

            if s == 1:
                out[:, 0, u * BS:(u + 1) * BS] = w[u]

    read_row(0)
    with jax.named_scope("update0"):
        update(0, a0, at0)
    read_row(1)
    with jax.named_scope("drain"):
        for pred, cp in pending[:sent_early]:
            pl.when(pred)(cp.wait_send)
    with jax.named_scope("update1"):
        update(1, a1, at1)
    with jax.named_scope("drain_late"):
        for pred, cp in pending[sent_early:]:
            pl.when(pred)(cp.wait_send)


def solution(mesh):
    rows, cols = mesh.shape["row"], mesh.shape["col"]

    def on_device(state, coupling, coupling_t, factor, cofactor, rates):
        slots = 2 * rows // cols
        width = slots * BS
        hbm = pl.BlockSpec(memory_space=pltpu.HBM)
        vmem = pl.BlockSpec(memory_space=pltpu.VMEM)
        f32, bf16 = jnp.float32, jnp.bfloat16
        dma = pltpu.SemaphoreType.DMA
        return pl.pallas_call(
            functools.partial(kernel, rows, cols, slots),
            out_shape=pltpu.VMEM((BS, 1, width), f32),
            in_specs=[hbm] * 6,
            out_specs=vmem,
            scratch_shapes=[
                pltpu.VMEM((BS, 1, width), f32),
                pltpu.VMEM((slots, BS, BS), f32),
                pltpu.VMEM((slots, BS, BS), bf16),
                pltpu.VMEM((slots, BS, BS), bf16),
                pltpu.VMEM((slots, BS, BS), bf16),
                pltpu.VMEM((slots, BS, BS), bf16),
                pltpu.VMEM((STEPS, 2, 2, BS, BS), f32),
                pltpu.VMEM((slots, 2, 8, BS), f32),
                pltpu.VMEM((slots, 1, BS), f32),
                pltpu.VMEM((slots, 8, BS), f32),
                pltpu.VMEM((STEPS, 8, BS), f32),
                pltpu.VMEM((STEPS, XS, QROWS + 8, BS), bf16),
                pltpu.VMEM((STEPS, slots, XS, QROWS + 8, BS), bf16),
                pltpu.VMEM((STEPS, 2, BS, BS), bf16),
                pltpu.VMEM((2, BS, BS), bf16),
                dma((4 + slots,)),
                dma((2, 2)),
                dma((STEPS, 2)),
                dma((STEPS,)),
                dma((STEPS,)),
                dma((slots,)),
                dma((slots,)),
                dma((slots,)),
                dma((slots,)),
                dma((slots,)),
                dma((slots,)),
                dma((STEPS, 8)),
                dma((STEPS,)),
                dma((STEPS, slots, rows // XS - 1 + XS - 1)),
                dma((STEPS, slots, XS)),
                dma((STEPS, 3 + XS)),
                dma((XS + 1,)),
                dma((2,)),
                dma((2,)),
                pltpu.SemaphoreType.REGULAR,
            ],
            compiler_params=pltpu.CompilerParams(
                collective_id=0, has_side_effects=True, vmem_limit_bytes=60000 * 1024
            ),
        )(
            state,
            coupling.reshape(BS, width),
            coupling_t.reshape(2, BS, width),
            factor.reshape(slots, 8, BS),
            cofactor.reshape(slots, 8, BS),
            rates,
        )

    return jax.shard_map(
        on_device,
        mesh=mesh,
        in_specs=(
            P("row", "col", None),
            P("row", "col", None),
            P(None, "row", "col", None),
            P(None, "col", "row", None),
            P(None, "col", "row", None),
            P(None, "col", None),
        ),
        out_specs=P("row", "col", None),
        check_vma=False,
    )
```

```python
import functools

import jax
import jax.numpy as jnp
from jax import lax
from jax.experimental import pallas as pl
from jax.experimental.pallas import tpu as pltpu
from jax.sharding import PartitionSpec as P

MESH = pl.DeviceIdType.MESH
STEPS = 2
XS = 4
BS = 256


def split2(a):
    hi = a.astype(jnp.bfloat16)
    return hi, (a - hi.astype(jnp.float32)).astype(jnp.bfloat16)


QROWS = BS // XS
TOP = 222.0


def bounds(a):
    largest = jnp.max(jnp.abs(a), axis=0, keepdims=True)
    return (jnp.maximum(largest, 1e-30) * 1.01).astype(jnp.bfloat16).astype(jnp.float32)


def encode(a, top):
    v = a * (TOP / top)
    p = v * v
    p = p * p
    p = p * p
    p = p * p
    return jnp.where(v < 0, -p, p).astype(jnp.bfloat16)


def decode(code, top):
    u = code.astype(jnp.float32)
    fourth = lax.rsqrt(lax.rsqrt(jnp.maximum(jnp.abs(u), 1.2e-38)))
    v = lax.rsqrt(lax.rsqrt(fourth)) * (top * (1.0 / TOP))
    return jnp.where(u < 0, -v, jnp.where(u > 0, v, 0.0))


def nn(a, b):
    return lax.dot_general(a, b, (((1,), (0,)), ((), ())), preferred_element_type=jnp.float32)


def nt(a, b):
    return lax.dot_general(a, b, (((1,), (1,)), ((), ())), preferred_element_type=jnp.float32)


def dot3(dot, a, b):
    ah, al = split2(a)
    bh, bl = split2(b)
    return dot(ah, bh) + dot(ah, bl) + dot(al, bh)


def kernel(
    rows, cols, slots,
    st_in, cp_in, ct_in, p_in, q_in, e_in, out,
    st, w, a0, a1, at0, at1, pq, own_pq, ev, es, el, xr, zs, xd, zd,
    loc_sem, pq_ssem, pq_rsem, e_ssem, e_rsem,
    at_ssem, at0_rsem, atf_ssem, at1_rsem, a1_ssem, a1_rsem,
    xr_ssem, xr_rsem, z_ssem, z_rsem, sv_ssem, er_ssem, fw_ssem, pq2_ssem, go_sem,
):
    r, c = lax.axis_index("row"), lax.axis_index("col")
    y, x = r // XS, lax.rem(r, XS)
    nb = 2 * rows
    pending = []

    def send(pred, src, dst, ssem, rsem, dev):
        cp = pltpu.make_async_remote_copy(
            src_ref=src, dst_ref=dst, send_sem=ssem, recv_sem=rsem,
            device_id=dev, device_id_type=MESH,
        )
        pl.when(pred)(cp.start)
        pending.append((pred, cp))

    def arrived(pred, dst, rsem):
        cp = pltpu.make_async_copy(dst, dst, rsem)
        pl.when(pred)(cp.wait)

    sc = [lax.rem(nb - 1 - s - r, cols) for s in range(STEPS)]
    us = [(nb - 1 - s - r) // cols for s in range(STEPS)]
    is_s = [c == sc[s] for s in range(STEPS)]
    tcol, tslot = lax.rem(r, cols), r // cols

    barrier = pltpu.get_barrier_semaphore()

    def greet(dr, dc):
        pl.semaphore_signal(barrier, inc=1, device_id=(dr, dc), device_id_type=MESH)

    ys = rows // XS
    for dx in range(1, XS):
        greet(y * XS + lax.rem(x + dx, XS), c)
    for dy in range(1, ys):
        greet(lax.rem(r + dy * XS, rows), c)
    greet(lax.rem(r + 1, rows), c)
    for dz in range(1, cols // 2):
        greet(r, lax.rem(c + 2 * dz, cols))
    greet(r, lax.rem(c + 1, cols))
    greet(r, c + 1 - 2 * lax.rem(c, 2))
    expected = XS - 1 + ys - 1 + 1 + cols // 2 - 1 + 2
    tj = y * XS + lax.rem(c, XS)
    near = lax.rem(y, cols // XS) == c // XS
    for s in range(STEPS):
        tj_col = lax.rem(nb - 1 - s - tj, cols)
        alone = (tj == r) & (tj_col == c)

        @pl.when(near & ~alone)
        def _(tj_col=tj_col):
            greet(tj, tj_col)

        expected = expected + jnp.where(is_s[s], XS, 0) - jnp.where(is_s[s] & (c == tcol), 1, 0)

        if s == 1:

            @pl.when(is_s[1] & (c != tcol))
            def _():
                greet(r, tcol)

            expected = expected + jnp.where((c == tcol) & (c != sc[1]), 1, 0)
            gathers = is_s[1] & (r < rows - 1)

            @pl.when(gathers)
            def _():
                for k in range(1, rows):
                    greet(lax.rem(r + k, rows), c)

            gatherers = jnp.where(c == cols - 1, 1, 2)
            expected = expected + gatherers - jnp.where(gathers, 1, 0)
            continue

        @pl.when(is_s[s])
        def _():
            for k in range(1, rows):
                greet(lax.rem(r + k, rows), c)

            for k in range(1, rows):
                greet(lax.rem(r + k, rows), tcol)

            @pl.when(c != tcol)
            def _():
                greet(r, tcol)

        expected = expected + 4 - jnp.where(is_s[s], 1, 0) - jnp.where(is_s[s] & (c == tcol), 1, 0)

    ld_st = pltpu.make_async_copy(st_in, st, loc_sem.at[0])
    ld_st.start()
    ld_a0 = [
        pltpu.make_async_copy(cp_in.at[:, pl.ds(u * BS, BS)], a0.at[u], loc_sem.at[1 + u])
        for u in range(slots)
    ]
    for cp in ld_a0:
        cp.start()
    ld_e = pltpu.make_async_copy(e_in, ev, loc_sem.at[1 + slots])
    ld_e.start()
    ld_pq = [
        pltpu.make_async_copy(ref, own_pq.at[:, t], loc_sem.at[2 + slots + t])
        for t, ref in enumerate((p_in, q_in))
    ]
    for cp in ld_pq:
        cp.start()
    ld_e.wait()
    for cp in ld_pq:
        cp.wait()
    es[...] = jnp.broadcast_to(ev[...], es.shape)
    with jax.named_scope("barrier"):
        pl.semaphore_wait(barrier, expected)

    def to_solver(side, q):
        slot = q + 2 * side
        m = c + cols * slot
        if side == 0:
            dr, dc = m, lax.rem(nb - 1 - m, cols)
        else:
            dr, dc = nb - 1 - m, c
        mine = (dr == r) & (dc == c)
        src = own_pq.at[slot]
        dst = pq.at[0, side, :, pl.ds(pl.multiple_of(r * 8, 8), 8), :]
        send(~mine, src, dst, pq_ssem.at[side, q], pq_rsem.at[0, side], (dr, dc))
        pl.when(mine)(pltpu.make_async_copy(src, dst, pq_rsem.at[0, side]).start)

    def to_second_solver(q):
        m = c + cols * (2 + q)
        dr = nb - 2 - m
        dr = jnp.where(c == cols - 1, nb - 2 - m, dr)
        on = dr >= 0
        mine = dr == r
        src = own_pq.at[2 + q]
        dst = pq.at[1, 1, :, pl.ds(pl.multiple_of(r * 8, 8), 8), :]
        send(on & ~mine, src, dst, pq2_ssem.at[q], pq_rsem.at[1, 1], (jnp.maximum(dr, 0), c))
        pl.when(on & mine)(pltpu.make_async_copy(src, dst, pq_rsem.at[1, 1]).start)

    def rate_to_solver(s):
        have = c == tcol
        mine = c == sc[s]
        send(have & ~mine, es.at[tslot], el.at[s], e_ssem.at[s], e_rsem.at[s], (r, sc[s]))
        pl.when(have & mine)(pltpu.make_async_copy(es.at[tslot], el.at[s], e_rsem.at[s]).start)

    for q in range(2):
        to_solver(0, q)
    in_plane = len(pending)
    for q in range(2):
        to_solver(1, q)
    for q in range(2):
        to_second_solver(q)
    for s in range(STEPS):
        rate_to_solver(s)

    def at_needed(g, u):
        m = c + cols * u
        return (m >= g - 1) & (m <= nb - 2 - g)

    g = lax.rem(r + rows // 2, rows)
    c_dn = lax.rem(c + cols - 1, cols)
    urgent = nb - 2 - g

    def step1_target(row, m):
        return (row <= m) & (row + m < nb - 2)

    def at_send(u, first):
        at_once = c + cols * u == urgent
        send(at_needed(g, u) & (at_once if first else ~at_once), ct_in.at[0, :, pl.ds(u * BS, BS)],
             at0.at[u], at_ssem.at[u], at0_rsem.at[u], (g, c))

    def bulk_sends(part):
        for u in part:
            at_send(u, False)

    def a1_sends():
        for u in range(slots):
            wrap = jnp.where(c == 0, 1, 0)
            du = u - wrap
            send((du >= 0) & step1_target(r, c_dn + cols * du), cp_in.at[:, pl.ds(u * BS, BS)],
                 a1.at[jnp.maximum(du, 0)], a1_ssem.at[u], a1_rsem.at[jnp.maximum(du, 0)], (r, c_dn))

    with jax.named_scope("pq_sent"):
        for dy in range(1, ys):
            pl.semaphore_signal(
                go_sem, inc=1, device_id=(lax.rem(r + dy * XS, rows), c), device_id_type=MESH
            )

    for u in range(1, slots):
        at_send(u, True)

    with jax.named_scope("local_in"):
        ld_st.wait()
        for u in range(slots):
            w[u] = st[:, 0, u * BS:(u + 1) * BS]
        for cp in ld_a0:
            cp.wait()

    def col_of(s, u):
        d = nb - 1 - s
        m = c + cols * u
        j = jnp.minimum(m, d - m)
        return d, m, j, m <= d

    def quarter(ref, q):
        return ref.at[q]

    def write_code(a, *refs):
        for q in range(XS):
            part = a[q * QROWS:(q + 1) * QROWS]
            top = bounds(part)
            code = encode(part, top)
            tops = jnp.broadcast_to(top, (8, BS)).astype(jnp.bfloat16)
            for ref in refs:
                ref[q, :QROWS] = code
                ref[q, QROWS:] = tops

    def read_code(ref, dst, order):
        for q in order:
            top = ref[q, QROWS:QROWS + 1, :].astype(jnp.float32)
            hi, lo = split2(decode(ref[q, :QROWS], top))
            dst[0, q * QROWS:(q + 1) * QROWS] = hi
            dst[1, q * QROWS:(q + 1) * QROWS] = lo

    def place(s, u):
        d = nb - 1 - s
        m = c + cols * u
        j = jnp.minimum(m, d - m)
        yj, xj = j // XS, lax.rem(j, XS)
        own_root = jnp.bool_(u >= 2) if isinstance(u, int) else u >= 2
        if s == 1:
            own_root = own_root | (lax.rem(j, cols // 2) == cols // 2 - 1)
        early = (j - 1) if s == 0 else j - 2 * rows
        early = jnp.where(u >= 2, early, -2 * rows)
        return j, yj, xj, m <= d, own_root, early

    def needed(s, u, row):
        j, yj, xj, valid, own_root, _ = place(s, u)
        return valid & ((row < j) | ((row == j) & ~own_root))

    def solver_sends(s):
        on = is_s[s]
        own = zs.at[s, us[s]]
        early = r - 1 if s == 0 else r - 2 * rows
        for k, dx in enumerate((3, 1, 2)):
            q = lax.rem(x + dx, XS)
            row = y * XS + q
            send(on & (row != early), quarter(own, q), quarter(own, q), sv_ssem.at[s, k],
                 z_rsem.at[s, us[s], q], (row, c))
        for q in range(XS):
            row = y * XS + q
            mine = (c == tcol) & (x == q)
            if s == 1:
                mine = mine | (r == rows - 1)
            send(on & ~mine, quarter(xr.at[s], q), quarter(zs.at[s, tslot], q), sv_ssem.at[s, 3 + q],
                 z_rsem.at[s, tslot, q], (row, tcol))

    def early_sends():
        on = is_s[0]
        send(on, xr.at[0], xr.at[0], er_ssem.at[XS], xr_rsem.at[0], (r, sc[1]))
        own = zs.at[0, us[0]]
        for q in range(XS):
            send(on & (r >= 1), quarter(own, q), quarter(own, q), er_ssem.at[q],
                 z_rsem.at[0, us[0], q], (jnp.maximum(r - 1, 0), c))

    def relay(s, u, on):
        j, yj, xj, valid, own_root, early = place(s, u)
        part = quarter(zs.at[s, u], x)
        first = on & valid & (y == yj)
        for y2 in range(ys - 1):
            row = y2 * XS + x
            send(first & (y2 < yj) & (row != early), part, part, z_ssem.at[s, u, y2],
                 z_rsem.at[s, u, x], (row, c))
        for k, dx in enumerate((1, 3, 2)):
            row = y * XS + lax.rem(x + dx, XS)
            send(on & needed(s, u, row) & (row != early), part, part, z_ssem.at[s, u, ys - 1 + k],
                 z_rsem.at[s, u, x], (row, c))

    def own_part(s, u):
        own = is_s[s] & (u == us[s])
        if s == 1:
            own = own | (is_s[s] & (c == tcol) & (u == tslot))
        return own

    def done_early(s, u):
        done = own_part(s, u)
        if s == 0:
            done = done | (is_s[1] & (u == u1) & (r < rows - 1))
        return done

    def relays(s, first, part=(3, 0, 2, 1)):
        for u in part:
            j, yj, xj, valid, own_root, early = place(s, u)
            on = valid & ((y == yj) if first else (y < yj)) & ~done_early(s, u)
            arrived(on, quarter(zs.at[s, u], x), z_rsem.at[s, u, x])
            relay(s, u, on)

    def rest(s, u):
        on = needed(s, u, r) & ~done_early(s, u)
        for k in range(1, XS):
            q = lax.rem(x + k, XS)
            arrived(on, quarter(zs.at[s, u], q), z_rsem.at[s, u, q])

    def row_sends(s):
        for dz in (4, 3, 5, 2, 6, 1, 7):
            send(is_s[s], xr.at[s], xr.at[s], xr_ssem.at[s, dz - 1], xr_rsem.at[s],
                 (r, lax.rem(c + 2 * dz, cols)))

    def row_relay(s):
        solver = is_s[s]
        early = is_s[1] if s == 0 else jnp.bool_(False)
        mate = c + 1 - 2 * lax.rem(c, 2)
        to_early = (mate == sc[1]) if s == 0 else jnp.bool_(False)
        member = lax.rem(c, 2) == lax.rem(sc[s], 2)
        arrived(~solver & ~early, xr.at[s], xr_rsem.at[s])
        send(member & ~to_early, xr.at[s], xr.at[s], xr_ssem.at[s, 7], xr_rsem.at[s], (r, mate))

    def solve(s):
        right = jnp.where(r == rows - 1, 0, 1) if s == 1 else 1
        left_e = jnp.transpose(el[s])[:, :1]
        right_e = ev[us[s]]
        mid = dot3(nn, pq[s, 0, 1], w[us[s]])
        mid = dot3(nt, mid, pq[s, right, 1])
        mid = mid / (left_e + right_e)
        mid = dot3(nn, pq[s, 0, 0], mid)
        sol = -dot3(nt, mid, pq[s, right, 0])
        if s == 0:
            write_code(sol, xr.at[s], zs.at[s, us[s]])
        else:
            write_code(sol, xr.at[s])
            last = r == rows - 1

            @pl.when(last)
            def _():
                write_code(jnp.transpose(sol), zs.at[s, us[s]])

            @pl.when(~last)
            def _():
                zs[s, us[s]] = xr[s]

            @pl.when(~last & (c == tcol))
            def _():
                zs[s, tslot] = xr[s]
        w[us[s]] = sol

    def terms(z, x_row, a, at, dot):
        return dot(a, z[0]) + dot(a, z[1]) + nn(x_row[0], at) + nn(x_row[1], at)

    u1 = us[1]
    def operators_ready(s):
        for side in range(2):
            on = is_s[s] & (r < rows - 1) if (s, side) == (1, 1) else is_s[s]
            arrived(on, pq.at[s, side], pq_rsem.at[s, side])
            if s == 0:
                to, dev = (on, (r, sc[1])) if side == 0 else (on & (x >= 9), (jnp.maximum(r - 1, 0), c))
                send(to, pq.at[0, side], pq.at[1, side], fw_ssem.at[side], pq_rsem.at[1, side], dev)
        arrived(is_s[s], el.at[s], e_rsem.at[s])

    with jax.named_scope("wait_pq00"):
        operators_ready(0)
    with jax.named_scope("solve0"):
        pl.when(is_s[0])(functools.partial(solve, 0))
    early_sends()
    solver_sends(0)
    relay(0, us[0], is_s[0])
    row_sends(0)
    with jax.named_scope("wait_go"):
        pl.semaphore_wait(go_sem, ys - 1)
    bulk_sends((3, 2, 1, 0))

    with jax.named_scope("early_wait_xr"):
        arrived(is_s[1], xr.at[0], xr_rsem.at[0])
    with jax.named_scope("early_wait_z"):
        early_on = is_s[1] & (r < rows - 1)
        for q in range(XS):
            arrived(early_on, quarter(zs.at[0, u1], q), z_rsem.at[0, u1, q])
        relay(0, u1, early_on)
    with jax.named_scope("early_wait_at"):
        arrived(is_s[1], at0.at[u1], at0_rsem.at[u1])

    @pl.when(is_s[1])
    def _():
        read_code(xr.at[0], xd.at[0], range(XS))

    @pl.when(is_s[1] & (r == rows - 1))
    def _():
        w[u1] = w[u1] - terms(xd.at[0], xd.at[0], a0[u1], at0[u1], nt)

    @pl.when(early_on)
    def _():
        read_code(zs.at[0, u1], zd, range(XS))
        w[u1] = w[u1] - terms(zd, xd.at[0], a0[u1], at0[u1], nn)

    with jax.named_scope("wait_pq1"):
        operators_ready(1)
    with jax.named_scope("solve1"):
        pl.when(is_s[1])(functools.partial(solve, 1))
    solver_sends(1)
    relay(1, u1, is_s[1])
    relay(1, tslot, is_s[1] & (c == tcol) & (r < rows - 1))
    row_sends(1)

    def at_forward(u):
        with jax.named_scope(f"at_forward{u}"):
            arrived(at_needed(r, u) & ~(is_s[1] & (u == u1)), at0.at[u], at0_rsem.at[u])
            send(at_needed(r, u) & (r >= 1), at0.at[u], at1.at[u], atf_ssem.at[u], at1_rsem.at[u],
                 (jnp.maximum(r - 1, 0), c))

    def step(name, *args):
        with jax.named_scope(name):
            relays(*args)

    at_forward(3)
    step("relay0a", 0, True)
    a1_sends()
    at_forward(2)
    step("relay0b_3", 0, False, (3,))
    step("relay0b_0", 0, False, (0,))
    step("relay1a", 1, True)
    sent_early = len(pending)
    at_forward(1)
    at_forward(0)
    step("relay0b_2", 0, False, (2,))
    step("relay0b_1", 0, False, (1,))
    step("relay1b_3", 1, False, (3,))
    step("relay1b_0", 1, False, (0,))
    step("relay1b_2", 1, False, (2,))
    step("relay1b_1", 1, False, (1,))
    with jax.named_scope("row0"):
        row_relay(0)
    with jax.named_scope("row1"):
        row_relay(1)
    def read_row(s):
        @pl.when(r <= nb - 2 - s - r)
        def _():
            read_code(xr.at[s], xd.at[s], range(XS))

    def update(s, a_ref, at_ref):
        for u in (3, 2, 0, 1) if s == 1 else (3, 0, 2, 1):
            m = c + cols * u
            target = (r <= m) & (r + m < nb - 1 - s)
            if s == 0:
                target = target & ~(is_s[1] & (u == u1))
            with jax.named_scope(f"rest{s}_{u}"):
                rest(s, u)
            if s == 1:
                with jax.named_scope(f"wait_at1_{u}"):
                    arrived(step1_target(r, m), a1.at[u], a1_rsem.at[u])
                    arrived(at_needed(r + 1, u) & (r < rows - 1), at1.at[u], at1_rsem.at[u])

            @pl.when(target)
            def _(u=u):
                read_code(zs.at[s, u], zd, range(XS))
                w[u] = w[u] - terms(zd, xd.at[s], a_ref[u], at_ref[u], nt if u < 2 else nn)

            if s == 1:
                out[:, 0, u * BS:(u + 1) * BS] = w[u]

    read_row(0)
    with jax.named_scope("update0"):
        update(0, a0, at0)
    read_row(1)
    with jax.named_scope("drain"):
        for pred, cp in pending[:sent_early]:
            pl.when(pred)(cp.wait_send)
    with jax.named_scope("update1"):
        update(1, a1, at1)
    with jax.named_scope("drain_late"):
        for pred, cp in pending[sent_early:]:
            pl.when(pred)(cp.wait_send)


def solution(mesh):
    rows, cols = mesh.shape["row"], mesh.shape["col"]

    def on_device(state, coupling, coupling_t, factor, cofactor, rates):
        slots = 2 * rows // cols
        width = slots * BS
        hbm = pl.BlockSpec(memory_space=pltpu.HBM)
        vmem = pl.BlockSpec(memory_space=pltpu.VMEM)
        f32, bf16 = jnp.float32, jnp.bfloat16
        dma = pltpu.SemaphoreType.DMA
        return pl.pallas_call(
            functools.partial(kernel, rows, cols, slots),
            out_shape=pltpu.VMEM((BS, 1, width), f32),
            in_specs=[hbm] * 6,
            out_specs=vmem,
            scratch_shapes=[
                pltpu.VMEM((BS, 1, width), f32),
                pltpu.VMEM((slots, BS, BS), f32),
                pltpu.VMEM((slots, BS, BS), bf16),
                pltpu.VMEM((slots, BS, BS), bf16),
                pltpu.VMEM((slots, BS, BS), bf16),
                pltpu.VMEM((slots, BS, BS), bf16),
                pltpu.VMEM((STEPS, 2, 2, BS, BS), f32),
                pltpu.VMEM((slots, 2, 8, BS), f32),
                pltpu.VMEM((slots, 1, BS), f32),
                pltpu.VMEM((slots, 8, BS), f32),
                pltpu.VMEM((STEPS, 8, BS), f32),
                pltpu.VMEM((STEPS, XS, QROWS + 8, BS), bf16),
                pltpu.VMEM((STEPS, slots, XS, QROWS + 8, BS), bf16),
                pltpu.VMEM((STEPS, 2, BS, BS), bf16),
                pltpu.VMEM((2, BS, BS), bf16),
                dma((4 + slots,)),
                dma((2, 2)),
                dma((STEPS, 2)),
                dma((STEPS,)),
                dma((STEPS,)),
                dma((slots,)),
                dma((slots,)),
                dma((slots,)),
                dma((slots,)),
                dma((slots,)),
                dma((slots,)),
                dma((STEPS, 8)),
                dma((STEPS,)),
                dma((STEPS, slots, rows // XS - 1 + XS - 1)),
                dma((STEPS, slots, XS)),
                dma((STEPS, 3 + XS)),
                dma((XS + 1,)),
                dma((2,)),
                dma((2,)),
                pltpu.SemaphoreType.REGULAR,
            ],
            compiler_params=pltpu.CompilerParams(
                collective_id=0, has_side_effects=True, vmem_limit_bytes=60000 * 1024
            ),
        )(
            state,
            coupling.reshape(BS, width),
            coupling_t.reshape(2, BS, width),
            factor.reshape(slots, 8, BS),
            cofactor.reshape(slots, 8, BS),
            rates,
        )

    return jax.shard_map(
        on_device,
        mesh=mesh,
        in_specs=(
            P("row", "col", None),
            P("row", "col", None),
            P(None, "row", "col", None),
            P(None, "col", "row", None),
            P(None, "col", "row", None),
            P(None, "col", None),
        ),
        out_specs=P("row", "col", None),
        check_vma=False,
    )
```
